128 devices in a mesh: wide: 64 (over x, y_hi, z, core), pair: 2 (over y_lo).
Axes of the slice: x: 4, y: 4 (y_hi: 2, y_lo: 2; y = y_hi * 2 + y_lo), z: 4, core: 2. Of those that a mesh axis runs over, the one named last changes fastest.
Arguments:
- pooled_b: bfloat16 [64, 64, 512, 128], P('wide', None, 'pair'), may hold values from -6 to 6
- dense_output_second: bfloat16 [32768, 128], P(('wide', 'pair')), may hold values from -4 to 4
- counts_b: int32 [32768, 26], P(('wide', 'pair')), may hold values from 1 to 8
- slot_of: int32 [64], replicated, may hold values from 0 to 63, each once
- stacked_a: bfloat16 [32768, 3456], P(('wide', 'pair')), may hold values from -4 to 4
- upstream_a: bfloat16 [32768, 3456], P(('wide', 'pair')), may hold values from -6 to 6
- counts_a: int32 [32768, 26], P(('wide', 'pair')), may hold values from 1 to 8
- down_projection: bfloat16 [3456, 512], P('wide'), may hold values from -0.109375 to 0.109375
- proj_up: bfloat16 [512, 3456], P(None, 'wide'), may hold values from -0.25 to 0.25
- cross_layer_bias: bfloat16 [3456], P('wide'), may hold values from -3 to 3
Outputs:
- crossed_b: bfloat16 [32768, 3456], P(('wide', 'pair'))
- dense_grad_a: bfloat16 [32768, 128], P(('wide', 'pair'))
- pooled_grad_a: bfloat16 [64, 64, 512, 128], P('wide', None, 'pair')
- grad_down: float32 [3456, 512], P('wide')
- grad_up: float32 [512, 3456], P(None, 'wide')
- grad_bias: float32 [3456], P('wide')
The draws below stay inside these ranges and needn't reach their ends.
Inputs may be any that keep to these rules, and one draw needn't show every extreme that they name: slot_of holds every slot once; its first 26 entries are the slots of tables 0 to 25, the rest are unused. Slot s lies on index s // 1 of wide.
All inputs are finite; a program needn't handle non-finite values.
Results may differ from the reference program's by a relative error of at most 0.0075.
Values may be sent and summed in bfloat16 or wider, within the bound.
A program may use at most 128 MiB of HBM per device.

```python
import jax
import jax.numpy as jnp
from jax import lax

E = 128
TABLES = 26
RANK = 512
SAMP = 256
POOL_MAX = 8
WIDTH = 3456
SLOTS = 64
BATCH = 32768
N_WIDE = 64
N_PAIR = 2


def touch_ends(drawn, stream_key, low, largest):
    dims = drawn.shape
    index_at = [jax.random.randint(jax.random.fold_in(stream_key, axis), (), 0, dims[axis]) for axis in range(len(dims))]
    drawn = drawn.at[tuple(index_at)].set(low)
    longest = dims.index(max(dims))
    index_at[longest] = (index_at[longest] + 1) % dims[longest]
    return drawn.at[tuple(index_at)].set(largest)


def raised(values, key, source, target, shards_of, factor):
    owner, partner = [(jnp.arange(values.shape[dim]) // (values.shape[dim] // shards_of)).reshape([-1 if axis == dim else 1 for axis in range(values.ndim)]) for dim in (source, target)]
    chosen = jax.random.permutation(key, shards_of)[partner]
    strong = (owner == chosen) | (owner == (partner + shards_of // 2) % shards_of)
    return jnp.where(strong, factor * values, values)


def block_scale(rng, extent, pieces, least, high):
    gain, own = 1.0, jax.random.fold_in(rng, 6)
    for axis_at, blocks in pieces:
        heights = jnp.exp(jax.random.uniform(jax.random.fold_in(own, axis_at), (blocks,), jnp.float32, least / len(pieces), high / len(pieces)))
        gain = gain * jnp.repeat(heights, extent[axis_at] // blocks).reshape([-1 if axis == axis_at else 1 for axis in range(len(extent))])
    return gain


def noise(rng, shape, spread, reach, split=(), kind=jnp.bfloat16):
    gain = block_scale(rng, shape, split, -0.22, 0.18) if split else 1.0
    drawn = jax.random.normal(rng, shape, jnp.float32) * spread * gain
    return jnp.minimum(jnp.maximum(drawn, -reach), reach).astype(kind)


def gaussian_with(key, dims, spread, limit, pieces, heavy, held_as=jnp.bfloat16):
    array = spread * jax.random.normal(key, dims, jnp.float32)
    if pieces:
        array = array * block_scale(key, dims, pieces, -0.22, 0.18)
    return jnp.clip(raised(array, jax.random.fold_in(key, 3), *heavy), -limit, limit).astype(held_as)


def setup_inputs(seed: int = 0) -> dict:
    keys = jax.random.split(jax.random.key(seed), 11)
    pooled_b = noise(keys[0], (SLOTS, N_WIDE, N_PAIR * SAMP, E), 1.0, 6.0, ((0, 64), (2, 2)))
    dense_output_second = noise(keys[1], (BATCH, E), 0.5, 4.0, ((0, 128),))
    counts_b = touch_ends(jax.random.randint(keys[2], (BATCH, TABLES), 1, POOL_MAX + 1), jax.random.fold_in(keys[2], 1), 1, POOL_MAX).astype(jnp.int32)
    slot_of = jax.random.permutation(keys[3], SLOTS).astype(jnp.int32)
    stacked_a = noise(keys[4], (BATCH, WIDTH), 0.5, 4.0, ((0, 128),))
    upstream_a = gaussian_with(keys[5], (BATCH, WIDTH), 0.25, 6.0, ((0, 128),), (0, 1, 128, 5.5))
    counts_a = touch_ends(jax.random.randint(keys[6], (BATCH, TABLES), 1, POOL_MAX + 1), jax.random.fold_in(keys[6], 1), 1, POOL_MAX).astype(jnp.int32)
    down_projection = noise(keys[7], (WIDTH, RANK), WIDTH ** -0.5, 0.109375, ((0, 64),))
    proj_up = noise(keys[8], (RANK, WIDTH), RANK ** -0.5, 0.25, ((1, 64),))
    cross_layer_bias = noise(keys[9], (WIDTH,), 0.5, 3.0, ((0, 64),))
    return {"pooled_b": pooled_b, "dense_output_second": dense_output_second, "counts_b": counts_b, "slot_of": slot_of, "stacked_a": stacked_a, "upstream_a": upstream_a, "counts_a": counts_a, "down_projection": down_projection, "proj_up": proj_up, "cross_layer_bias": cross_layer_bias}


def table_means(slot_rows, lookup_count, table_slots):
    picked = jnp.take(slot_rows, table_slots, axis=0).astype(jnp.float32)
    scaled = picked / jnp.transpose(lookup_count).astype(jnp.float32)[:, :, None]
    return jnp.transpose(scaled, (1, 0, 2)).reshape(scaled.shape[1], -1).astype(jnp.bfloat16)


def cross_forward(stacked, down, up):
    low_rank = jnp.dot(stacked, down, preferred_element_type=jnp.float32).astype(jnp.bfloat16)
    projected = jnp.dot(low_rank, up, preferred_element_type=jnp.float32)
    return low_rank, projected


def crossed_output(stacked, projected, bias):
    stacked_wide = stacked.astype(jnp.float32)
    return (stacked_wide * (projected + bias.astype(jnp.float32)) + stacked_wide).astype(jnp.bfloat16)


def cross_backward(stacked, upstream, lookup_count, down, up, bias, feature_index):
    low_rank, projected = cross_forward(stacked, down, up)
    stacked_wide = stacked.astype(jnp.float32)
    upstream_wide = upstream.astype(jnp.float32)
    scale_grad = upstream_wide * stacked_wide
    grad_bias = jnp.sum(scale_grad, axis=0)
    proj_grad = scale_grad.astype(jnp.bfloat16)
    over_rows = (((0,), (0,)), ((), ()))
    over_cols = (((1,), (1,)), ((), ()))
    grad_up = lax.dot_general(low_rank, proj_grad, over_rows, preferred_element_type=jnp.float32)
    low_grad = lax.dot_general(proj_grad, up, over_cols, preferred_element_type=jnp.float32).astype(jnp.bfloat16)
    grad_down = lax.dot_general(stacked, low_grad, over_rows, preferred_element_type=jnp.float32)
    input_grad = upstream_wide * (projected + bias.astype(jnp.float32)) + upstream_wide
    input_grad = input_grad + lax.dot_general(low_grad, down, over_cols, preferred_element_type=jnp.float32)
    rows = stacked.shape[0]
    dense_gradient = input_grad[:, :feature_index].astype(jnp.bfloat16)
    table_gradient = input_grad[:, feature_index:].reshape(rows, -1, feature_index) / lookup_count.astype(jnp.float32)[:, :, None]
    table_gradient = jnp.transpose(table_gradient, (1, 0, 2)).astype(jnp.bfloat16)
    return dense_gradient, table_gradient, grad_down, grad_up, grad_bias


def reference(pooled_b, dense_output_second, counts_b, slot_of, stacked_a, upstream_a, counts_a, down_projection, proj_up, cross_layer_bias):
    feature_index = dense_output_second.shape[1]
    table_slots = slot_of[:TABLES].astype(jnp.int32)
    slot_rows = pooled_b.reshape(SLOTS, BATCH, feature_index)

    def per_block(running, block_index):
        first_row = (block_index * SAMP).astype(jnp.int32)
        rows_b = lax.dynamic_slice_in_dim(slot_rows, first_row, SAMP, 1)
        dense_rows = lax.dynamic_slice_in_dim(dense_output_second, first_row, SAMP, 0)
        counts_rows_b = lax.dynamic_slice_in_dim(counts_b, first_row, SAMP, 0)
        stacked_b = jnp.concatenate([dense_rows, table_means(rows_b, counts_rows_b, table_slots)], axis=1)
        low_rank, projected = cross_forward(stacked_b, down_projection, proj_up)
        crossed = crossed_output(stacked_b, projected, cross_layer_bias)
        stacked_rows = lax.dynamic_slice_in_dim(stacked_a, first_row, SAMP, 0)
        upstream_rows = lax.dynamic_slice_in_dim(upstream_a, first_row, SAMP, 0)
        counts_rows_a = lax.dynamic_slice_in_dim(counts_a, first_row, SAMP, 0)
        dense_gradient, table_gradient, grad_d, grad_u, grad_b = cross_backward(
            stacked_rows, upstream_rows, counts_rows_a, down_projection, proj_up, cross_layer_bias, feature_index)
        slot_grad = jnp.zeros((SLOTS, SAMP, feature_index), jnp.bfloat16).at[table_slots].set(table_gradient)
        running = (running[0] + grad_d, running[1] + grad_u, running[2] + grad_b)
        return running, (crossed, dense_gradient, slot_grad)

    initial = (jnp.zeros((WIDTH, RANK), jnp.float32), jnp.zeros((RANK, WIDTH), jnp.float32),
               jnp.zeros((WIDTH,), jnp.float32))
    blocks = jnp.arange(BATCH // SAMP, dtype=jnp.int32)
    totals, (crossed, dense_gradient, slot_grad) = lax.scan(per_block, initial, blocks)
    crossed_b = crossed.reshape(BATCH, WIDTH)
    dense_grad_a = dense_gradient.reshape(BATCH, feature_index)
    pooled_grad_a = jnp.transpose(slot_grad, (1, 0, 2, 3)).reshape(SLOTS, N_WIDE, N_PAIR * SAMP, feature_index)
    return crossed_b, dense_grad_a, pooled_grad_a, totals[0], totals[1], totals[2]
```

```python
import functools

import jax
import jax.numpy as jnp
from jax import lax
from jax.experimental import pallas as pl
from jax.experimental.pallas import tpu as pltpu
from jax.sharding import PartitionSpec as P

MESH = pl.DeviceIdType.MESH
F32 = jnp.float32
BF16 = jnp.bfloat16

ROWS = 54
PAD = 56
RANK = 512
E = 128
TABLES = 26
SLOTS = 64
SAMP = 256
WIDTH = 3456
BLK = 384
OVER_ROWS = (((0,), (0,)), ((), ()))
OVER_COLS = (((1,), (1,)), ((), ()))


def place():
    w = lax.axis_index("wide")
    yl = lax.axis_index("pair")
    return w // 16, (w // 8) % 2, yl, (w // 2) % 4, w % 2


def device(x, yh, yl, z, c):
    return (((x * 2 + yh) * 4 + z) * 2 + c, yl)


def along_a(x, yh, yl, z, c, d):
    return device((x + d * (1 - c)) % 4, yh, yl, (z + d * c) % 4, c)


def along_b(x, yh, yl, z, c, d):
    return device((x + d * c) % 4, yh, yl, (z + d * (1 - c)) % 4, c)


def meet(devices):
    barrier = pltpu.get_barrier_semaphore()
    for d in devices:
        pl.semaphore_signal(barrier, inc=1, device_id=d, device_id_type=MESH)
    pl.semaphore_wait(barrier, len(devices))


def gather_kernel(shard, full, send, recv, local_sem):
    x, yh, yl, z, c = place()
    o = 1 - c
    b = z * o + x * c
    a = x * o + z * c
    k = yh * 2 + c
    sib = device(x, yh, yl, z, o)
    part = [device(x, 1 - yh, 1 - yl, z, i) for i in range(2)]
    a_next, a_prev = along_a(x, yh, yl, z, c, 1), along_a(x, yh, yl, z, c, 3)
    b_next, b_prev = along_b(x, yh, yl, z, c, 1), along_b(x, yh, yl, z, c, 3)
    meet([sib, part[0], part[1], a_next, a_prev, b_next, b_prev])
    n = [0]
    started = []

    def copy(src, dst, to, slot):
        cp = pltpu.make_async_remote_copy(
            src_ref=src,
            dst_ref=dst,
            send_sem=send.at[n[0]],
            recv_sem=recv.at[slot],
            device_id=to,
            device_id_type=MESH,
        )
        n[0] += 1
        started.append(cp)
        cp.start()
        return cp

    mine = pltpu.make_async_copy(shard.at[c], full.at[c, b, a, k], local_sem)
    mine.start()
    s1 = []
    for i in range(2):
        bi, ai = (z, x) if i == 0 else (x, z)
        slot = 1 + (c + i) % 2
        s1.append(copy(shard.at[i], full.at[i, bi, ai, k], part[i], slot))
    s1.append(copy(shard.at[o], full.at[o, a, b, k], sib, 0))
    mine.wait()
    for cp in s1:
        cp.wait_recv()
    a_m, a_p, a_o = (a + 3) % 4, (a + 1) % 4, (a + 2) % 4
    b_m, b_p, b_o = (b + 3) % 4, (b + 1) % 4, (b + 2) % 4
    lo, hi = pl.ds(0, 2), pl.ds(2, 2)

    def block(bb, aa):
        return full.at[c, bb, aa]

    def half(bb, aa, h):
        return full.at[c, bb, aa, h]

    up = copy(block(b, a), block(b, a), a_next, 3)
    down = copy(block(b, a), block(b, a), a_prev, 4)
    outer = []

    def out(j, aa):
        outer.append(
            (
                aa,
                copy(block(b, aa), block(b, aa), b_next, 7 + 4 * j),
                copy(block(b, aa), block(b, aa), b_prev, 8 + 4 * j),
                9 + 4 * j,
            )
        )

    across = []

    def over(bb, aa, j):
        across.append(copy(block(bb, aa), block(bb, aa), sib, 23 + j))

    out(0, a)
    up.wait_recv()
    up2 = copy(half(b, a_m, lo), half(b, a_m, lo), a_next, 5)
    out(1, a_m)
    down.wait_recv()
    down2 = copy(half(b, a_p, hi), half(b, a_p, hi), a_prev, 6)
    out(2, a_p)
    over(b, a, 0)
    over(b, a_m, 1)
    over(b, a_p, 2)
    up2.wait_recv()
    down2.wait_recv()
    out(3, a_o)
    over(b, a_o, 3)
    far = []
    for j, (aa, u, d, slot) in enumerate(outer):
        u.wait_recv()
        u2 = copy(half(b_m, aa, lo), half(b_m, aa, lo), b_next, slot)
        over(b_m, aa, 4 + j)
        d.wait_recv()
        d2 = copy(half(b_p, aa, hi), half(b_p, aa, hi), b_prev, slot + 1)
        over(b_p, aa, 8 + j)
        far.append((aa, u2, d2))
    for j, (aa, u2, d2) in enumerate(far):
        u2.wait_recv()
        d2.wait_recv()
        over(b_o, aa, 12 + j)
    for cp in across:
        cp.wait_recv()
    for cp in started:
        cp.wait_send()


N_GATHER = 3 + 4 + 16 + 16


def gather_weights(shard):
    return pl.pallas_call(
        gather_kernel,
        out_shape=jax.ShapeDtypeStruct((2, 4, 4, 4, PAD, RANK), BF16),
        in_specs=[pl.BlockSpec(memory_space=pl.ANY)],
        out_specs=pl.BlockSpec(memory_space=pltpu.VMEM),
        scratch_shapes=[
            pltpu.SemaphoreType.DMA((N_GATHER,)),
            pltpu.SemaphoreType.DMA((N_GATHER,)),
            pltpu.SemaphoreType.DMA,
        ],
        compiler_params=pltpu.CompilerParams(
            collective_id=1, has_side_effects=True, vmem_limit_bytes=24 << 20
        ),
        name="gather_weights",
    )(shard)


def reduce_kernel(g, out, sibling, mid_p, mid_m, end_p, end_m, total, imid, iend, inner, last,
                  send, recv):
    x, yh, yl, z, c = place()
    o = 1 - c
    b = z * o + x * c
    a = x * o + z * c
    sib = device(x, yh, yl, z, o)
    a_next, a_prev = along_a(x, yh, yl, z, c, 1), along_a(x, yh, yl, z, c, 3)
    b_next, b_prev = along_b(x, yh, yl, z, c, 1), along_b(x, yh, yl, z, c, 3)
    y = yh * 2 + yl
    column = []
    for d in range(1, 4):
        yy = (y + d) % 4
        for i in range(2):
            column.append((d, yy, i, device(x, yy // 2, yy % 2, z, i)))
    meet([sib, a_next, a_prev, b_next, b_prev] + [t[3] for t in column])
    n = [0]
    started = []

    def copy(src, dst, to, slot=None):
        cp = pltpu.make_async_remote_copy(
            src_ref=src,
            dst_ref=dst,
            send_sem=send.at[n[0]],
            recv_sem=recv.at[n[0] if slot is None else slot],
            device_id=to,
            device_id_type=MESH,
        )
        n[0] += 1
        started.append(cp)
        cp.start()
        return cp

    steps = (2, 1, 3, 0)
    lo, hi = pl.ds(0, 2), pl.ds(2, 2)
    crossing = {}
    for db in steps:
        for da in steps:
            bb, aa = (a + db) % 4, (b + da) % 4
            crossing[db, da] = copy(g.at[o, bb, aa], sibling.at[bb, aa], sib)
    got = set()

    def mine(db, da, h):
        if (db, da) not in got:
            crossing[db, da].wait_recv()
            got.add((db, da))
        bb, aa = (b + db) % 4, (a + da) % 4
        return g[c, bb, aa, h].astype(F32) + sibling[bb, aa, h].astype(F32)

    def keep(db, da, h, value):
        sibling[(b + db) % 4, (a + da) % 4, h] = value.astype(BF16)

    def at(db, da, h):
        return sibling.at[(b + db) % 4, (a + da) % 4, h]

    all_k = pl.ds(0, 4)
    first = {}
    for j, da in enumerate(steps):
        keep(2, da, all_k, mine(2, da, all_k))
        first[da] = (
            copy(at(2, da, lo), mid_p.at[j], b_next),
            copy(at(2, da, hi), mid_m.at[j], b_prev),
        )
    second = {}
    for j, da in enumerate(steps):
        p, m = first[da]
        keep(1, da, hi, mine(1, da, hi))
        keep(3, da, lo, mine(3, da, lo))
        p.wait_recv()
        keep(1, da, lo, mine(1, da, lo) + mid_p[j].astype(F32))
        sp = copy(at(1, da, all_k), end_p.at[j], b_next)
        m.wait_recv()
        keep(3, da, hi, mine(3, da, hi) + mid_m[j].astype(F32))
        sm = copy(at(3, da, all_k), end_m.at[j], b_prev)
        second[da] = (sp, sm)

    def summed(j, da):
        p, m = second[da]
        own = mine(0, da, all_k)
        p.wait_recv()
        own = own + end_p[j].astype(F32)
        m.wait_recv()
        return own + end_m[j].astype(F32)

    total[0] = summed(0, 2).astype(BF16)
    fp = copy(total.at[0, lo], imid.at[0], a_next)
    fm = copy(total.at[0, hi], imid.at[1], a_prev)
    near_p = summed(1, 1)
    near_m = summed(2, 3)
    total[1, hi] = near_p[2:4].astype(BF16)
    total[2, lo] = near_m[0:2].astype(BF16)
    fp.wait_recv()
    total[1, lo] = (near_p[0:2] + imid[0].astype(F32)).astype(BF16)
    gp = copy(total.at[1], iend.at[0], a_next)
    fm.wait_recv()
    total[2, hi] = (near_m[2:4] + imid[1].astype(F32)).astype(BF16)
    gm = copy(total.at[2], iend.at[1], a_prev)
    own = summed(3, 0)
    gp.wait_recv()
    own = own + iend[0].astype(F32)
    gm.wait_recv()
    own = own + iend[1].astype(F32)
    inner[...] = own.astype(BF16)
    base = n[0]
    for d, yy, i, to in column:
        copy(inner.at[(yy // 2) * 2 + i], last.at[d, c], to, base + 2 * (d - 1) + c)
    copy(inner.at[yh * 2 + o], last.at[0, c], sib).wait_recv()
    ready = inner[yh * 2 + c].astype(F32)
    for d in range(1, 4):
        for i in range(2):
            pltpu.make_async_remote_copy(
                src_ref=inner.at[0],
                dst_ref=last.at[d, i],
                send_sem=send.at[0],
                recv_sem=recv.at[base + 2 * (d - 1) + i],
                device_id=sib,
                device_id_type=MESH,
            ).wait_recv()
    for i in range(2):
        far = last[1, i].astype(F32) + last[2, i].astype(F32) + last[3, i].astype(F32)
        near = jnp.where(c == i, ready, last[0, i].astype(F32))
        out[i] = far + near
    for cp in started:
        cp.wait_send()


N_REDUCE = 16 + 8 + 8 + 4 + 7


def reduce_gradients(g):
    half = (2, PAD, RANK)
    whole = (4, PAD, RANK)
    return pl.pallas_call(
        reduce_kernel,
        out_shape=jax.ShapeDtypeStruct((2, PAD, RANK), F32),
        in_specs=[pl.BlockSpec(memory_space=pltpu.VMEM)],
        out_specs=pl.BlockSpec(memory_space=pltpu.VMEM),
        scratch_shapes=[
            pltpu.VMEM((4, 4) + whole, BF16),
            pltpu.VMEM((4,) + half, BF16),
            pltpu.VMEM((4,) + half, BF16),
            pltpu.VMEM((4,) + whole, BF16),
            pltpu.VMEM((4,) + whole, BF16),
            pltpu.VMEM((3,) + whole, BF16),
            pltpu.VMEM((2,) + half, BF16),
            pltpu.VMEM((2,) + whole, BF16),
            pltpu.VMEM(whole, BF16),
            pltpu.VMEM((4, 2, PAD, RANK), BF16),
            pltpu.SemaphoreType.DMA((N_REDUCE,)),
            pltpu.SemaphoreType.DMA((N_REDUCE,)),
        ],
        compiler_params=pltpu.CompilerParams(
            collective_id=2, has_side_effects=True, vmem_limit_bytes=40 << 20
        ),
        name="reduce_gradients",
    )(g)


def shard_of(m, w):
    x, yh, z, c = w // 16, (w // 8) % 2, (w // 2) % 4, w % 2
    return (m, z, x, yh * 2 + c) if m == 0 else (m, x, z, yh * 2 + c)


def backward_kernel(slots, full, stacked, upstream, counts, v, u, bias, dense, slot_grad, g,
                    pg, gv, gu, gb):
    for w in range(64):
        rows = slice(ROWS * w, ROWS * (w + 1))
        v[rows, :] = full[shard_of(0, w)][0:ROWS]
        u[rows, :] = full[shard_of(1, w)][0:ROWS]
        bias[0:1, rows] = full[shard_of(0, w)][ROWS : ROWS + 1, 0:ROWS].astype(F32)
    low = jnp.zeros((SAMP, RANK), F32)
    lg = jnp.zeros((SAMP, RANK), F32)
    for j in range(WIDTH // BLK):
        cols = slice(BLK * j, BLK * (j + 1))
        st = stacked[:, cols]
        scale = upstream[:, cols].astype(F32) * st.astype(F32)
        gb[0:1, cols] = jnp.sum(scale, axis=0, keepdims=True)
        p = scale.astype(BF16)
        pg[:, cols] = p
        low = low + jnp.dot(st, v[cols, :], preferred_element_type=F32)
        lg = lg + jnp.dot(p, u[cols, :], preferred_element_type=F32)
    low = low.astype(BF16)
    lg = lg.astype(BF16)
    slot_grad[...] = jnp.zeros_like(slot_grad)
    inverse = 1.0 / counts[...].astype(F32)
    for j in range(WIDTH // BLK):
        cols = slice(BLK * j, BLK * (j + 1))
        up = upstream[:, cols].astype(F32)
        projected = lax.dot_general(low, u[cols, :], OVER_COLS, preferred_element_type=F32)
        through = lax.dot_general(lg, v[cols, :], OVER_COLS, preferred_element_type=F32)
        grad = up * (projected + bias[0:1, cols]) + up + through
        for i in range(BLK // E):
            t = j * (BLK // E) + i - 1
            piece = grad[:, E * i : E * (i + 1)]
            if t < 0:
                dense[...] = piece.astype(BF16)
            else:
                slot_grad[slots[t]] = (piece * inverse[:, t : t + 1]).astype(BF16)
        gu[cols, :] = lax.dot_general(
            pg[:, cols], low, OVER_ROWS, preferred_element_type=F32
        ).astype(BF16)
        gv[cols, :] = lax.dot_general(
            stacked[:, cols], lg, OVER_ROWS, preferred_element_type=F32
        ).astype(BF16)
    for w in range(64):
        rows = slice(ROWS * w, ROWS * (w + 1))
        g[shard_of(0, w) + (slice(0, ROWS),)] = gv[rows, :]
        g[shard_of(1, w) + (slice(0, ROWS),)] = gu[rows, :]
        g[shard_of(0, w) + (slice(ROWS, ROWS + 1), slice(0, ROWS))] = gb[0:1, rows].astype(BF16)


def backward(full, stacked, upstream, counts, slots):
    vmem = pl.BlockSpec(memory_space=pltpu.VMEM)
    return pl.pallas_call(
        backward_kernel,
        out_shape=(
            jax.ShapeDtypeStruct((WIDTH, RANK), BF16),
            jax.ShapeDtypeStruct((WIDTH, RANK), BF16),
            jax.ShapeDtypeStruct((1, WIDTH), F32),
            jax.ShapeDtypeStruct((SAMP, E), BF16),
            jax.ShapeDtypeStruct((SLOTS, SAMP, E), BF16),
            jax.ShapeDtypeStruct((2, 4, 4, 4, PAD, RANK), BF16),
        ),
        in_specs=[pl.BlockSpec(memory_space=pltpu.SMEM)] + [vmem] * 4,
        out_specs=[vmem] * 6,
        scratch_shapes=[
            pltpu.VMEM((SAMP, WIDTH), BF16),
            pltpu.VMEM((WIDTH, RANK), BF16),
            pltpu.VMEM((WIDTH, RANK), BF16),
            pltpu.VMEM((1, WIDTH), F32),
        ],
        compiler_params=pltpu.CompilerParams(vmem_limit_bytes=60 << 20),
        cost_estimate=pl.CostEstimate(
            flops=6 * 2 * SAMP * WIDTH * RANK, bytes_accessed=40 << 20, transcendentals=0
        ),
        name="backward_a",
    )(slots, full, stacked, upstream, counts)


def forward_kernel(slots, arrived, dense, counts, v, u, bias, crossed, st):
    inverse = 1.0 / counts[...].astype(F32)
    st[:, 0:E] = dense[...]
    for t in range(TABLES):
        mean = arrived[slots[t]].astype(F32) * inverse[:, t : t + 1]
        st[:, E * (t + 1) : E * (t + 2)] = mean.astype(BF16)
    low = jnp.zeros((SAMP, RANK), F32)
    for j in range(WIDTH // BLK):
        cols = slice(BLK * j, BLK * (j + 1))
        low = low + jnp.dot(st[:, cols], v[cols, :], preferred_element_type=F32)
    low = low.astype(BF16)
    for j in range(WIDTH // BLK):
        cols = slice(BLK * j, BLK * (j + 1))
        wide = st[:, cols].astype(F32)
        projected = lax.dot_general(low, u[cols, :], OVER_COLS, preferred_element_type=F32)
        crossed[:, cols] = (wide * (projected + bias[0:1, cols]) + wide).astype(BF16)


def forward(arrived, dense, counts, slots, v, u, bias):
    vmem = pl.BlockSpec(memory_space=pltpu.VMEM)
    return pl.pallas_call(
        forward_kernel,
        out_shape=jax.ShapeDtypeStruct((SAMP, WIDTH), BF16),
        in_specs=[pl.BlockSpec(memory_space=pltpu.SMEM)] + [vmem] * 6,
        out_specs=vmem,
        scratch_shapes=[pltpu.VMEM((SAMP, WIDTH), BF16)],
        compiler_params=pltpu.CompilerParams(vmem_limit_bytes=40 << 20),
        cost_estimate=pl.CostEstimate(
            flops=2 * 2 * SAMP * WIDTH * RANK, bytes_accessed=16 << 20, transcendentals=0
        ),
        name="forward_b",
    )(slots, arrived, dense, counts, v, u, bias)


def local(
    pooled_b,
    dense_output_second,
    counts_b,
    slot_of,
    stacked_a,
    upstream_a,
    counts_a,
    down_projection,
    proj_up,
    cross_layer_bias,
):
    slots = slot_of[:TABLES]
    arrived = lax.all_to_all(pooled_b, "wide", split_axis=1, concat_axis=0, tiled=True)
    bias_row = jnp.pad(cross_layer_bias[None, :], ((0, 1), (0, RANK - ROWS)))
    shard = jnp.stack(
        [
            jnp.concatenate([down_projection, bias_row], axis=0),
            jnp.pad(jnp.transpose(proj_up), ((0, PAD - ROWS), (0, 0))),
        ]
    )
    full = gather_weights(shard)
    v, u, bias, dense_gradient, slot_grad, g = backward(
        full, stacked_a, upstream_a, counts_a, slots
    )
    returned = lax.all_to_all(
        slot_grad.reshape(SLOTS, 1, SAMP, E), "wide", split_axis=0, concat_axis=1, tiled=True
    )
    sums = reduce_gradients(g)
    crossed_b = forward(
        arrived.reshape(SLOTS, SAMP, E), dense_output_second, counts_b, slots, v, u, bias
    )
    return (
        crossed_b,
        dense_gradient,
        returned,
        sums[0, :ROWS],
        jnp.transpose(sums[1, :ROWS]),
        sums[0, ROWS, :ROWS],
    )


def solution(mesh):
    return jax.shard_map(
        local,
        mesh=mesh,
        in_specs=(
            P("wide", None, "pair", None),
            P(("wide", "pair"), None),
            P(("wide", "pair"), None),
            P(),
            P(("wide", "pair"), None),
            P(("wide", "pair"), None),
            P(("wide", "pair"), None),
            P("wide", None),
            P(None, "wide"),
            P("wide"),
        ),
        out_specs=(
            P(("wide", "pair"), None),
            P(("wide", "pair"), None),
            P("wide", None, "pair", None),
            P("wide", None),
            P(None, "wide"),
            P("wide"),
        ),
        check_vma=False,
    )
```

```python
import itertools

import jax
import jax.numpy as jnp
from jax import lax
from jax.experimental import pallas as pl
from jax.experimental.pallas import tpu as pltpu
from jax.sharding import PartitionSpec as P

MESH = pl.DeviceIdType.MESH
F32 = jnp.float32
BF16 = jnp.bfloat16

ROWS = 54
PAD = 56
RANK = 512
E = 128
TABLES = 26
SLOTS = 64
SAMP = 256
WIDTH = 3456
BLK = 384
OVER_ROWS = (((0,), (0,)), ((), ()))
OVER_COLS = (((1,), (1,)), ((), ()))


def place():
    w = lax.axis_index("wide")
    yl = lax.axis_index("pair")
    return w // 16, (w // 8) % 2, yl, (w // 2) % 4, w % 2


def device(x, yh, yl, z, c):
    return (((x * 2 + yh) * 4 + z) * 2 + c, yl)


def along_a(x, yh, yl, z, c, d):
    return device((x + d * (1 - c)) % 4, yh, yl, (z + d * c) % 4, c)


def along_b(x, yh, yl, z, c, d):
    return device((x + d * c) % 4, yh, yl, (z + d * (1 - c)) % 4, c)


def load_of(offset):
    dx, dy, dz, _ = offset
    loads = [0] * 6
    for d, at in ((dx, 0), (dz, 2)):
        if d % 2:
            loads[at + (d == 3)] += 1
        elif d:
            loads[at] += 1
            loads[at + 1] += 1
    if dy:
        loads[4] += 1
        loads[5] += 1
    return loads


def exchange_order():
    left = [o for o in itertools.product(range(4), range(2), range(4), range(2)) if any(o)]
    total, order = [0] * 6, []
    while left:

        def cost(offset):
            after = [p + q for p, q in zip(total, load_of(offset))]
            return max(after) - min(after), -sum(load_of(offset))

        best = min(left, key=cost)
        left.remove(best)
        order.append(best)
        total = [p + q for p, q in zip(total, load_of(best))]
    return order


ORDER = exchange_order()
N_GATHER = 3 + 4 + 16 + 16
N_REDUCE = 16 + 8 + 8 + 4 + 7
FEED_B = (0, 4, 4, 4, 4, 4, 4, 4, 4)
FEED_A = (8, 4, 4, 4, 4, 4, 4, 4, 4, 4)


def target(me, offset):
    x, yh, _, z, c = me
    dx, dy, dz, dc = offset
    sx = dx + ((4 - dx) % 4 - dx) * c
    sz = dz + ((4 - dz) % 4 - dz) * c
    return ((((x + sx) % 4) * 2 + (yh + dy) % 2) * 4 + (z + sz) % 4) * 2 + (c + dc) % 2


def shard_of(m, w):
    x, yh, z, c = w // 16, (w // 8) % 2, (w // 2) % 4, w % 2
    return (m, z, x, yh * 2 + c) if m == 0 else (m, x, z, yh * 2 + c)


def step_kernel(slots, index, pooled, shard, stacked_h, upstream_h, counts_a_h, dense_h, counts_b_h,
                crossed_h, dense_g, returned, out,
                full, v, u, bias, stacked, upstream, pg, gv, gu, gb, tg, snd, arrived, st, counts_a,
                counts_b, sibling, mid_p, mid_m, end_p, end_m, total, imid, iend, inner, last,
                gsend, grecv, rsend, rrecv, local_sem, bsend, brecv, asend, arecv):
    place_of = place()
    x, yh, yl, z, c = place_of
    me = lax.axis_index("wide")
    o = 1 - c
    b = z * o + x * c
    a = x * o + z * c
    k = yh * 2 + c
    y = yh * 2 + yl
    sib = device(x, yh, yl, z, o)
    part = [device(x, 1 - yh, 1 - yl, z, i) for i in range(2)]
    a_next, a_prev = along_a(x, yh, yl, z, c, 1), along_a(x, yh, yl, z, c, 3)
    b_next, b_prev = along_b(x, yh, yl, z, c, 1), along_b(x, yh, yl, z, c, 3)
    lo, hi, all_k = pl.ds(0, 2), pl.ds(2, 2), pl.ds(0, 4)

    def load(src, dst, i):
        cp = pltpu.make_async_copy(src, dst, local_sem.at[i])
        cp.start()
        return cp

    loads = [
        load(stacked_h, stacked, 0),
        load(upstream_h, upstream, 1),
        load(counts_a_h, counts_a, 2),
        load(counts_b_h, counts_b, 3),
        load(dense_h, st.at[:, pl.ds(0, E)], 4),
    ]
    mine_b = load(pooled.at[me], arrived.at[me], 5)
    mine_w = load(shard.at[c], full.at[c, b, a, k], 6)

    barrier = pltpu.get_barrier_semaphore()

    @pl.loop(0, SLOTS)
    def _(i):
        @pl.when(i != me)
        def _():
            pl.semaphore_signal(barrier, inc=1, device_id=(i, yl), device_id_type=MESH)

    for d in (1, 3):
        for i in range(2):
            yy = (y + d) % 4
            pl.semaphore_signal(
                barrier, inc=1, device_id=device(x, yy // 2, yy % 2, z, i), device_id_type=MESH
            )
    pl.semaphore_wait(barrier, SLOTS - 1 + 4)

    fed = [0, 0]

    def feed_b(count):
        for offset in ORDER[fed[0] : fed[0] + count]:
            to = target(place_of, offset)
            pltpu.make_async_remote_copy(
                src_ref=pooled.at[to],
                dst_ref=arrived.at[me],
                send_sem=bsend,
                recv_sem=brecv,
                device_id=(to, yl),
                device_id_type=MESH,
            ).start()
        fed[0] += count

    def feed_a(count):
        for offset in ORDER[fed[1] : fed[1] + count]:
            to = target(place_of, offset)
            pltpu.make_async_remote_copy(
                src_ref=snd.at[to],
                dst_ref=returned.at[me],
                send_sem=asend,
                recv_sem=arecv,
                device_id=(to, yl),
                device_id_type=MESH,
            ).start()
        fed[1] += count

    n = [0]
    started = []

    def gcopy(src, dst, to, slot):
        cp = pltpu.make_async_remote_copy(
            src_ref=src,
            dst_ref=dst,
            send_sem=gsend.at[n[0]],
            recv_sem=grecv.at[slot],
            device_id=to,
            device_id_type=MESH,
        )
        n[0] += 1
        started.append(cp)
        cp.start()
        return cp

    s1 = []
    for i in range(2):
        bi, ai = (z, x) if i == 0 else (x, z)
        s1.append(gcopy(shard.at[i], full.at[i, bi, ai, k], part[i], 1 + (c + i) % 2))
    s1.append(gcopy(shard.at[o], full.at[o, a, b, k], sib, 0))
    feed_b(FEED_B[0])
    mine_w.wait()
    for cp in s1:
        cp.wait_recv()
    a_m, a_p, a_o = (a + 3) % 4, (a + 1) % 4, (a + 2) % 4
    b_m, b_p, b_o = (b + 3) % 4, (b + 1) % 4, (b + 2) % 4

    def ring(at, aa, to, slot, h=all_k):
        return gcopy(full.at[c, at, aa, h], full.at[c, at, aa, h], to, slot)

    outer = []

    def out_ring(j, aa):
        nxt = ring(b, aa, b_next, 7 + 4 * j)
        prv = ring(b, aa, b_prev, 8 + 4 * j)
        outer.append((aa, nxt, prv, 9 + 4 * j))

    across = []

    def over(bb, aa, j):
        across.append(ring(bb, aa, sib, 23 + j))

    up = ring(b, a, a_next, 3)
    down = ring(b, a, a_prev, 4)
    out_ring(0, a)
    feed_b(FEED_B[1])
    up.wait_recv()
    up2 = ring(b, a_m, a_next, 5, lo)
    out_ring(1, a_m)
    down.wait_recv()
    down2 = ring(b, a_p, a_prev, 6, hi)
    out_ring(2, a_p)
    over(b, a, 0)
    over(b, a_m, 1)
    over(b, a_p, 2)
    feed_b(FEED_B[2])
    up2.wait_recv()
    down2.wait_recv()
    out_ring(3, a_o)
    over(b, a_o, 3)
    feed_b(FEED_B[3])
    far = []
    for j, (aa, nxt, prv, slot) in enumerate(outer):
        nxt.wait_recv()
        n2 = ring(b_m, aa, b_next, slot, lo)
        over(b_m, aa, 4 + j)
        prv.wait_recv()
        p2 = ring(b_p, aa, b_prev, slot + 1, hi)
        over(b_p, aa, 8 + j)
        far.append((aa, n2, p2))
        feed_b(FEED_B[4 + j])
    for j, (aa, n2, p2) in enumerate(far):
        n2.wait_recv()
        p2.wait_recv()
        over(b_o, aa, 12 + j)
    feed_b(FEED_B[8])
    for cp in across:
        cp.wait_recv()
    for cp in started:
        cp.wait_send()
    feed_b(len(ORDER) - fed[0])

    for cp in loads[:3]:
        cp.wait()
    for w in range(64):
        rows = slice(ROWS * w, ROWS * (w + 1))
        v[rows, :] = full[shard_of(0, w)][0:ROWS]
        u[rows, :] = full[shard_of(1, w)][0:ROWS]
        bias[0:1, rows] = full[shard_of(0, w)][ROWS : ROWS + 1, 0:ROWS].astype(F32)
    low = jnp.zeros((SAMP, RANK), F32)
    lg = jnp.zeros((SAMP, RANK), F32)
    for j in range(WIDTH // BLK):
        cols = slice(BLK * j, BLK * (j + 1))
        sa = stacked[:, cols]
        scale = upstream[:, cols].astype(F32) * sa.astype(F32)
        gb[0:1, cols] = jnp.sum(scale, axis=0, keepdims=True)
        p = scale.astype(BF16)
        pg[:, cols] = p
        low = low + jnp.dot(sa, v[cols, :], preferred_element_type=F32)
        lg = lg + jnp.dot(p, u[cols, :], preferred_element_type=F32)
    low = low.astype(BF16)
    lg = lg.astype(BF16)
    tg[0] = jnp.zeros((SAMP, E), BF16)
    inverse = (1.0 / counts_a[...].astype(F32)).T
    for j in range(WIDTH // BLK):
        cols = slice(BLK * j, BLK * (j + 1))
        ua = upstream[:, cols].astype(F32)
        projected = lax.dot_general(low, u[cols, :], OVER_COLS, preferred_element_type=F32)
        through = lax.dot_general(lg, v[cols, :], OVER_COLS, preferred_element_type=F32)
        grad = ua * (projected + bias[0:1, cols]) + ua + through
        for i in range(BLK // E):
            t = j * (BLK // E) + i
            piece = grad[:, E * i : E * (i + 1)]
            if t == 0:
                dense_g[...] = piece.astype(BF16)
            else:
                tg[t] = (piece * inverse[:, t - 1 : t]).astype(BF16)
        gu[cols, :] = lax.dot_general(
            pg[:, cols], low, OVER_ROWS, preferred_element_type=F32
        ).astype(BF16)
        gv[cols, :] = lax.dot_general(
            stacked[:, cols], lg, OVER_ROWS, preferred_element_type=F32
        ).astype(BF16)
    for w in range(64):
        rows = slice(ROWS * w, ROWS * (w + 1))
        full[shard_of(0, w) + (slice(0, ROWS),)] = gv[rows, :]
        full[shard_of(1, w) + (slice(0, ROWS),)] = gu[rows, :]
        full[shard_of(0, w) + (slice(ROWS, ROWS + 1), slice(0, ROWS))] = gb[0:1, rows].astype(BF16)

    m = [0]
    sent = []

    def rcopy(src, dst, to, slot=None):
        cp = pltpu.make_async_remote_copy(
            src_ref=src,
            dst_ref=dst,
            send_sem=rsend.at[m[0]],
            recv_sem=rrecv.at[m[0] if slot is None else slot],
            device_id=to,
            device_id_type=MESH,
        )
        m[0] += 1
        sent.append(cp)
        cp.start()
        return cp

    steps = (2, 1, 3, 0)
    crossing = {}
    for db in steps:
        for da in steps:
            bb, aa = (a + db) % 4, (b + da) % 4
            crossing[db, da] = rcopy(full.at[o, bb, aa], sibling.at[bb, aa], sib)

    for s in range(SLOTS):
        snd[s] = tg[index[s]]
    got = set()

    def mine(db, da, h):
        if (db, da) not in got:
            crossing[db, da].wait_recv()
            got.add((db, da))
        bb, aa = (b + db) % 4, (a + da) % 4
        return full[c, bb, aa, h].astype(F32) + sibling[bb, aa, h].astype(F32)

    def keep(db, da, h, value):
        sibling[(b + db) % 4, (a + da) % 4, h] = value.astype(BF16)

    def at(db, da, h):
        return sibling.at[(b + db) % 4, (a + da) % 4, h]

    first = {}
    for j, da in enumerate(steps):
        keep(2, da, all_k, mine(2, da, all_k))
        first[da] = (
            rcopy(at(2, da, lo), mid_p.at[j], b_next),
            rcopy(at(2, da, hi), mid_m.at[j], b_prev),
        )
    home_a = load(snd.at[me], returned.at[me], 7)
    feed_a(FEED_A[0])
    second = {}
    for j, da in enumerate(steps):
        p, q = first[da]
        keep(1, da, hi, mine(1, da, hi))
        keep(3, da, lo, mine(3, da, lo))
        p.wait_recv()
        keep(1, da, lo, mine(1, da, lo) + mid_p[j].astype(F32))
        sp = rcopy(at(1, da, all_k), end_p.at[j], b_next)
        q.wait_recv()
        keep(3, da, hi, mine(3, da, hi) + mid_m[j].astype(F32))
        sm = rcopy(at(3, da, all_k), end_m.at[j], b_prev)
        second[da] = (sp, sm)
        feed_a(FEED_A[1 + j])

    def summed(j, da):
        p, q = second[da]
        own = mine(0, da, all_k)
        p.wait_recv()
        own = own + end_p[j].astype(F32)
        q.wait_recv()
        return own + end_m[j].astype(F32)

    total[0] = summed(0, 2).astype(BF16)
    fp = rcopy(total.at[0, lo], imid.at[0], a_next)
    fm = rcopy(total.at[0, hi], imid.at[1], a_prev)
    feed_a(FEED_A[5])
    near_p = summed(1, 1)
    near_m = summed(2, 3)
    total[1, hi] = near_p[2:4].astype(BF16)
    total[2, lo] = near_m[0:2].astype(BF16)
    fp.wait_recv()
    total[1, lo] = (near_p[0:2] + imid[0].astype(F32)).astype(BF16)
    gp = rcopy(total.at[1], iend.at[0], a_next)
    fm.wait_recv()
    total[2, hi] = (near_m[2:4] + imid[1].astype(F32)).astype(BF16)
    gm = rcopy(total.at[2], iend.at[1], a_prev)
    feed_a(FEED_A[6])
    own = summed(3, 0)
    gp.wait_recv()
    own = own + iend[0].astype(F32)
    gm.wait_recv()
    own = own + iend[1].astype(F32)
    inner[...] = own.astype(BF16)
    base = m[0]
    for d in range(1, 4):
        for i in range(2):
            yy = (y + d) % 4
            rcopy(
                inner.at[(yy // 2) * 2 + i],
                last.at[d, c],
                device(x, yy // 2, yy % 2, z, i),
                base + 2 * (d - 1) + c,
            )
    near = rcopy(inner.at[yh * 2 + o], last.at[0, c], sib)
    feed_a(len(ORDER) - fed[1])

    def await_exchange(send, recv, buf):
        cp = pltpu.make_async_remote_copy(
            src_ref=buf.at[pl.ds(0, SLOTS - 1)],
            dst_ref=buf.at[pl.ds(0, SLOTS - 1)],
            send_sem=send,
            recv_sem=recv,
            device_id=sib,
            device_id_type=MESH,
        )
        cp.wait_send()
        cp.wait_recv()

    for cp in loads[3:]:
        cp.wait()
    mine_b.wait()
    await_exchange(bsend, brecv, arrived)
    inverse_b = (1.0 / counts_b[...].astype(F32)).T
    for t in range(TABLES):
        mean = arrived[slots[t]].astype(F32) * inverse_b[:, t : t + 1]
        st[:, E * (t + 1) : E * (t + 2)] = mean.astype(BF16)
    low_b = jnp.zeros((SAMP, RANK), F32)
    for j in range(WIDTH // BLK):
        cols = slice(BLK * j, BLK * (j + 1))
        low_b = low_b + jnp.dot(st[:, cols], v[cols, :], preferred_element_type=F32)
    low_b = low_b.astype(BF16)
    for j in range(WIDTH // BLK):
        cols = slice(BLK * j, BLK * (j + 1))
        wide = st[:, cols].astype(F32)
        projected = lax.dot_general(low_b, u[cols, :], OVER_COLS, preferred_element_type=F32)
        st[:, cols] = (wide * (projected + bias[0:1, cols]) + wide).astype(BF16)
    write = load(st, crossed_h, 8)

    near.wait_recv()
    for d in range(1, 4):
        for i in range(2):
            pltpu.make_async_remote_copy(
                src_ref=inner.at[0],
                dst_ref=last.at[d, i],
                send_sem=rsend.at[0],
                recv_sem=rrecv.at[base + 2 * (d - 1) + i],
                device_id=sib,
                device_id_type=MESH,
            ).wait_recv()
    ready = inner[k].astype(F32)
    for i in range(2):
        others = last[1, i].astype(F32) + last[2, i].astype(F32) + last[3, i].astype(F32)
        out[i] = others + jnp.where(c == i, ready, last[0, i].astype(F32))
    for cp in sent:
        cp.wait_send()
    home_a.wait()
    write.wait()
    await_exchange(asend, arecv, returned)


def step(slots, index, pooled, shard, stacked, upstream, counts_a, dense, counts_b):
    smem = pl.BlockSpec(memory_space=pltpu.SMEM)
    vmem = pl.BlockSpec(memory_space=pltpu.VMEM)
    anywhere = pl.BlockSpec(memory_space=pl.ANY)
    half = (2, PAD, RANK)
    whole = (4, PAD, RANK)
    return pl.pallas_call(
        step_kernel,
        out_shape=(
            jax.ShapeDtypeStruct((SAMP, WIDTH), BF16),
            jax.ShapeDtypeStruct((SAMP, E), BF16),
            jax.ShapeDtypeStruct((SLOTS, SAMP, E), BF16),
            jax.ShapeDtypeStruct((2, PAD, RANK), F32),
        ),
        in_specs=[smem] * 2 + [anywhere] * 7,
        out_specs=[anywhere, vmem, anywhere, vmem],
        scratch_shapes=[
            pltpu.VMEM((2, 4, 4, 4, PAD, RANK), BF16),
            pltpu.VMEM((WIDTH, RANK), BF16),
            pltpu.VMEM((WIDTH, RANK), BF16),
            pltpu.VMEM((1, WIDTH), F32),
            pltpu.VMEM((SAMP, WIDTH), BF16),
            pltpu.VMEM((SAMP, WIDTH), BF16),
            pltpu.VMEM((SAMP, WIDTH), BF16),
            pltpu.VMEM((WIDTH, RANK), BF16),
            pltpu.VMEM((WIDTH, RANK), BF16),
            pltpu.VMEM((1, WIDTH), F32),
            pltpu.VMEM((TABLES + 1, SAMP, E), BF16),
            pltpu.VMEM((SLOTS, SAMP, E), BF16),
            pltpu.VMEM((SLOTS, SAMP, E), BF16),
            pltpu.VMEM((SAMP, WIDTH), BF16),
            pltpu.VMEM((TABLES, SAMP), jnp.int32),
            pltpu.VMEM((TABLES, SAMP), jnp.int32),
            pltpu.VMEM((4, 4) + whole, BF16),
            pltpu.VMEM((4,) + half, BF16),
            pltpu.VMEM((4,) + half, BF16),
            pltpu.VMEM((4,) + whole, BF16),
            pltpu.VMEM((4,) + whole, BF16),
            pltpu.VMEM((3,) + whole, BF16),
            pltpu.VMEM((2,) + half, BF16),
            pltpu.VMEM((2,) + whole, BF16),
            pltpu.VMEM(whole, BF16),
            pltpu.VMEM((4, 2, PAD, RANK), BF16),
            pltpu.SemaphoreType.DMA((N_GATHER,)),
            pltpu.SemaphoreType.DMA((N_GATHER,)),
            pltpu.SemaphoreType.DMA((N_REDUCE,)),
            pltpu.SemaphoreType.DMA((N_REDUCE,)),
            pltpu.SemaphoreType.DMA((9,)),
            pltpu.SemaphoreType.DMA,
            pltpu.SemaphoreType.DMA,
            pltpu.SemaphoreType.DMA,
            pltpu.SemaphoreType.DMA,
        ],
        compiler_params=pltpu.CompilerParams(
            collective_id=1, has_side_effects=True, vmem_limit_bytes=62 << 20
        ),
        name="cross_step",
    )(slots, index, pooled, shard, stacked, upstream, counts_a, dense, counts_b)


def local(
    pooled_b,
    dense_output_second,
    counts_b,
    slot_of,
    stacked_a,
    upstream_a,
    counts_a,
    down_projection,
    proj_up,
    cross_layer_bias,
):
    slots = slot_of[:TABLES]
    held = slots[None, :] == jnp.arange(SLOTS, dtype=jnp.int32)[:, None]
    index = jnp.sum(jnp.where(held, jnp.arange(1, TABLES + 1, dtype=jnp.int32), 0), axis=1)
    bias_row = jnp.pad(cross_layer_bias[None, :], ((0, 1), (0, RANK - ROWS)))
    shard = jnp.stack(
        [
            jnp.concatenate([down_projection, bias_row], axis=0),
            jnp.pad(jnp.transpose(proj_up), ((0, PAD - ROWS), (0, 0))),
        ]
    )
    crossed_b, dense_gradient, returned, sums = step(
        slots,
        index,
        pooled_b[0],
        shard,
        stacked_a,
        upstream_a,
        jnp.transpose(counts_a),
        dense_output_second,
        jnp.transpose(counts_b),
    )
    return (
        crossed_b,
        dense_gradient,
        returned[None],
        sums[0, :ROWS],
        jnp.transpose(sums[1, :ROWS]),
        sums[0, ROWS, :ROWS],
    )


def solution(mesh):
    return jax.shard_map(
        local,
        mesh=mesh,
        in_specs=(
            P("wide", None, "pair", None),
            P(("wide", "pair"), None),
            P(("wide", "pair"), None),
            P(),
            P(("wide", "pair"), None),
            P(("wide", "pair"), None),
            P(("wide", "pair"), None),
            P("wide", None),
            P(None, "wide"),
            P("wide"),
        ),
        out_specs=(
            P(("wide", "pair"), None),
            P(("wide", "pair"), None),
            P("wide", None, "pair", None),
            P("wide", None),
            P(None, "wide"),
            P("wide"),
        ),
        check_vma=False,
    )
```

```python
import itertools

import jax
import jax.numpy as jnp
from jax import lax
from jax.experimental import pallas as pl
from jax.experimental.pallas import tpu as pltpu
from jax.sharding import PartitionSpec as P

MESH = pl.DeviceIdType.MESH
F32 = jnp.float32
BF16 = jnp.bfloat16

ROWS = 54
PAD = 56
RANK = 512
E = 128
TABLES = 26
SLOTS = 64
SAMP = 256
WIDTH = 3456
BLK = 384
OVER_ROWS = (((0,), (0,)), ((), ()))
OVER_COLS = (((1,), (1,)), ((), ()))


def place():
    w = lax.axis_index("wide")
    yl = lax.axis_index("pair")
    return w // 16, (w // 8) % 2, yl, (w // 2) % 4, w % 2


def device(x, yh, yl, z, c):
    return (((x * 2 + yh) * 4 + z) * 2 + c, yl)


def along_a(x, yh, yl, z, c, d):
    return device((x + d * (1 - c)) % 4, yh, yl, (z + d * c) % 4, c)


def along_b(x, yh, yl, z, c, d):
    return device((x + d * c) % 4, yh, yl, (z + d * (1 - c)) % 4, c)


def load_of(offset):
    dx, dy, dz, _ = offset
    loads = [0] * 6
    for d, at in ((dx, 0), (dz, 2)):
        if d % 2:
            loads[at + (d == 3)] += 1
        elif d:
            loads[at] += 1
            loads[at + 1] += 1
    if dy:
        loads[4] += 1
        loads[5] += 1
    return loads


def exchange_order():
    left = [o for o in itertools.product(range(4), range(2), range(4), range(2)) if any(o)]
    total, order = [0] * 6, []
    while left:

        def cost(offset):
            after = [p + q for p, q in zip(total, load_of(offset))]
            return max(after) - min(after), -sum(load_of(offset))

        best = min(left, key=cost)
        left.remove(best)
        order.append(best)
        total = [p + q for p, q in zip(total, load_of(best))]
    return order


ORDER = exchange_order()
N_GATHER = 3 + 4 + 16 + 16
N_REDUCE = 16 + 8 + 8 + 4 + 7
FEED_B = (0, 4, 4, 4, 4, 4, 4, 4, 4)
FEED_A = (8, 4, 4, 4, 4, 4, 4, 4, 4, 4)


def target(me, offset):
    x, yh, _, z, c = me
    dx, dy, dz, dc = offset
    sx = dx + ((4 - dx) % 4 - dx) * c
    sz = dz + ((4 - dz) % 4 - dz) * c
    return ((((x + sx) % 4) * 2 + (yh + dy) % 2) * 4 + (z + sz) % 4) * 2 + (c + dc) % 2


def shard_of(m, w):
    x, yh, z, c = w // 16, (w // 8) % 2, (w // 2) % 4, w % 2
    return (m, z, x, yh * 2 + c) if m == 0 else (m, x, z, yh * 2 + c)


def step_kernel(slots, pooled, down_h, up_h, bias_h, stacked_h, upstream_h, counts_a_h, dense_h, counts_b_h,
                crossed_h, dense_g, returned, out,
                index, raw, raw_bias, shard, full, v, u, bias, stacked, upstream, pg, gv, gu, gb, tg, snd, arrived, st, counts_a,
                counts_b, sibling, mid_p, mid_m, end_p, end_m, total, imid, iend, inner, last,
                gsend, grecv, rsend, rrecv, local_sem, bsend, brecv, asend, arecv):
    place_of = place()
    x, yh, yl, z, c = place_of
    me = lax.axis_index("wide")
    o = 1 - c
    b = z * o + x * c
    a = x * o + z * c
    k = yh * 2 + c
    y = yh * 2 + yl
    sib = device(x, yh, yl, z, o)
    part = [device(x, 1 - yh, 1 - yl, z, i) for i in range(2)]
    a_next, a_prev = along_a(x, yh, yl, z, c, 1), along_a(x, yh, yl, z, c, 3)
    b_next, b_prev = along_b(x, yh, yl, z, c, 1), along_b(x, yh, yl, z, c, 3)
    lo, hi, all_k = pl.ds(0, 2), pl.ds(2, 2), pl.ds(0, 4)

    def load(src, dst, i):
        cp = pltpu.make_async_copy(src, dst, local_sem.at[i])
        cp.start()
        return cp

    loads = [
        load(stacked_h, stacked, 0),
        load(upstream_h, upstream, 1),
        load(counts_a_h, counts_a, 2),
        load(counts_b_h, counts_b, 3),
        load(dense_h, st.at[:, pl.ds(0, E)], 4),
    ]
    mine_b = load(pooled.at[me], arrived.at[me], 5)
    raws = [load(down_h, raw.at[0], 6), load(up_h, raw.at[1], 9), load(bias_h, raw_bias, 10)]

    barrier = pltpu.get_barrier_semaphore()

    @pl.loop(0, SLOTS)
    def _(i):
        @pl.when(i != me)
        def _():
            pl.semaphore_signal(barrier, inc=1, device_id=(i, yl), device_id_type=MESH)

    for d in (1, 3):
        for i in range(2):
            yy = (y + d) % 4
            pl.semaphore_signal(
                barrier, inc=1, device_id=device(x, yy // 2, yy % 2, z, i), device_id_type=MESH
            )
    shard[...] = jnp.zeros_like(shard)
    for cp in raws:
        cp.wait()
    for i in range(2):
        shard[i, 0:ROWS] = raw[i]
    shard[0, ROWS : ROWS + 1, 0:ROWS] = raw_bias[...]
    pl.semaphore_wait(barrier, SLOTS - 1 + 4)

    fed = [0, 0]

    def feed_b(count):
        for offset in ORDER[fed[0] : fed[0] + count]:
            to = target(place_of, offset)
            pltpu.make_async_remote_copy(
                src_ref=pooled.at[to],
                dst_ref=arrived.at[me],
                send_sem=bsend,
                recv_sem=brecv,
                device_id=(to, yl),
                device_id_type=MESH,
            ).start()
        fed[0] += count

    def feed_a(count):
        for offset in ORDER[fed[1] : fed[1] + count]:
            to = target(place_of, offset)
            pltpu.make_async_remote_copy(
                src_ref=snd.at[to],
                dst_ref=returned.at[me],
                send_sem=asend,
                recv_sem=arecv,
                device_id=(to, yl),
                device_id_type=MESH,
            ).start()
        fed[1] += count

    n = [0]
    started = []

    def gcopy(src, dst, to, slot):
        cp = pltpu.make_async_remote_copy(
            src_ref=src,
            dst_ref=dst,
            send_sem=gsend.at[n[0]],
            recv_sem=grecv.at[slot],
            device_id=to,
            device_id_type=MESH,
        )
        n[0] += 1
        started.append(cp)
        cp.start()
        return cp

    s1 = []
    for i in range(2):
        bi, ai = (z, x) if i == 0 else (x, z)
        s1.append(gcopy(shard.at[i], full.at[i, bi, ai, k], part[i], 1 + (c + i) % 2))
    s1.append(gcopy(shard.at[o], full.at[o, a, b, k], sib, 0))
    feed_b(FEED_B[0])

    @pl.loop(0, SLOTS)
    def _(s):
        held = jnp.int32(0)
        for t in range(TABLES):
            held = jnp.where(slots[t] == s, t + 1, held)
        index[s] = held

    full[c, b, a, k] = shard[c]
    for cp in s1:
        cp.wait_recv()
    a_m, a_p, a_o = (a + 3) % 4, (a + 1) % 4, (a + 2) % 4
    b_m, b_p, b_o = (b + 3) % 4, (b + 1) % 4, (b + 2) % 4

    def ring(at, aa, to, slot, h=all_k):
        return gcopy(full.at[c, at, aa, h], full.at[c, at, aa, h], to, slot)

    outer = []

    def out_ring(j, aa):
        nxt = ring(b, aa, b_next, 7 + 4 * j)
        prv = ring(b, aa, b_prev, 8 + 4 * j)
        outer.append((aa, nxt, prv, 9 + 4 * j))

    across = []

    def over(bb, aa, j):
        across.append(ring(bb, aa, sib, 23 + j))

    up = ring(b, a, a_next, 3)
    down = ring(b, a, a_prev, 4)
    out_ring(0, a)
    feed_b(FEED_B[1])
    up.wait_recv()
    up2 = ring(b, a_m, a_next, 5, lo)
    out_ring(1, a_m)
    down.wait_recv()
    down2 = ring(b, a_p, a_prev, 6, hi)
    out_ring(2, a_p)
    over(b, a, 0)
    over(b, a_m, 1)
    over(b, a_p, 2)
    feed_b(FEED_B[2])
    up2.wait_recv()
    down2.wait_recv()
    out_ring(3, a_o)
    over(b, a_o, 3)
    feed_b(FEED_B[3])
    far = []
    for j, (aa, nxt, prv, slot) in enumerate(outer):
        nxt.wait_recv()
        n2 = ring(b_m, aa, b_next, slot, lo)
        over(b_m, aa, 4 + j)
        prv.wait_recv()
        p2 = ring(b_p, aa, b_prev, slot + 1, hi)
        over(b_p, aa, 8 + j)
        far.append((aa, n2, p2))
        feed_b(FEED_B[4 + j])
    for j, (aa, n2, p2) in enumerate(far):
        n2.wait_recv()
        p2.wait_recv()
        over(b_o, aa, 12 + j)
    feed_b(FEED_B[8])
    for cp in across:
        cp.wait_recv()
    for cp in started:
        cp.wait_send()
    feed_b(len(ORDER) - fed[0])

    for cp in loads[:3]:
        cp.wait()
    for w in range(64):
        rows = slice(ROWS * w, ROWS * (w + 1))
        v[rows, :] = full[shard_of(0, w)][0:ROWS]
        u[rows, :] = full[shard_of(1, w)][0:ROWS]
        bias[0:1, rows] = full[shard_of(0, w)][ROWS : ROWS + 1, 0:ROWS].astype(F32)
    low = jnp.zeros((SAMP, RANK), F32)
    lg = jnp.zeros((SAMP, RANK), F32)
    for j in range(WIDTH // BLK):
        cols = slice(BLK * j, BLK * (j + 1))
        sa = stacked[:, cols]
        scale = upstream[:, cols].astype(F32) * sa.astype(F32)
        gb[0:1, cols] = jnp.sum(scale, axis=0, keepdims=True)
        p = scale.astype(BF16)
        pg[:, cols] = p
        low = low + jnp.dot(sa, v[cols, :], preferred_element_type=F32)
        lg = lg + jnp.dot(p, u[cols, :], preferred_element_type=F32)
    low = low.astype(BF16)
    lg = lg.astype(BF16)
    tg[0] = jnp.zeros((SAMP, E), BF16)
    inverse = (1.0 / counts_a[...].astype(F32)).T
    for j in range(WIDTH // BLK):
        cols = slice(BLK * j, BLK * (j + 1))
        ua = upstream[:, cols].astype(F32)
        projected = lax.dot_general(low, u[cols, :], OVER_COLS, preferred_element_type=F32)
        through = lax.dot_general(lg, v[cols, :], OVER_COLS, preferred_element_type=F32)
        grad = ua * (projected + bias[0:1, cols]) + ua + through
        for i in range(BLK // E):
            t = j * (BLK // E) + i
            piece = grad[:, E * i : E * (i + 1)]
            if t == 0:
                dense_g[...] = piece.astype(BF16)
            else:
                tg[t] = (piece * inverse[:, t - 1 : t]).astype(BF16)
        gu[cols, :] = lax.dot_general(
            pg[:, cols], low, OVER_ROWS, preferred_element_type=F32
        ).astype(BF16)
        gv[cols, :] = lax.dot_general(
            stacked[:, cols], lg, OVER_ROWS, preferred_element_type=F32
        ).astype(BF16)
    for w in range(64):
        rows = slice(ROWS * w, ROWS * (w + 1))
        full[shard_of(0, w) + (slice(0, ROWS),)] = gv[rows, :]
        full[shard_of(1, w) + (slice(0, ROWS),)] = gu[rows, :]
        full[shard_of(0, w) + (slice(ROWS, ROWS + 1), slice(0, ROWS))] = gb[0:1, rows].astype(BF16)

    m = [0]
    sent = []

    def rcopy(src, dst, to, slot=None):
        cp = pltpu.make_async_remote_copy(
            src_ref=src,
            dst_ref=dst,
            send_sem=rsend.at[m[0]],
            recv_sem=rrecv.at[m[0] if slot is None else slot],
            device_id=to,
            device_id_type=MESH,
        )
        m[0] += 1
        sent.append(cp)
        cp.start()
        return cp

    steps = (2, 1, 3, 0)
    crossing = {}
    for db in steps:
        for da in steps:
            bb, aa = (a + db) % 4, (b + da) % 4
            crossing[db, da] = rcopy(full.at[o, bb, aa], sibling.at[bb, aa], sib)

    for s in range(SLOTS):
        snd[s] = tg[index[s]]
    got = set()

    def mine(db, da, h):
        if (db, da) not in got:
            crossing[db, da].wait_recv()
            got.add((db, da))
        bb, aa = (b + db) % 4, (a + da) % 4
        return full[c, bb, aa, h].astype(F32) + sibling[bb, aa, h].astype(F32)

    def keep(db, da, h, value):
        sibling[(b + db) % 4, (a + da) % 4, h] = value.astype(BF16)

    def at(db, da, h):
        return sibling.at[(b + db) % 4, (a + da) % 4, h]

    first = {}
    for j, da in enumerate(steps):
        keep(2, da, all_k, mine(2, da, all_k))
        first[da] = (
            rcopy(at(2, da, lo), mid_p.at[j], b_next),
            rcopy(at(2, da, hi), mid_m.at[j], b_prev),
        )
    home_a = load(snd.at[me], returned.at[me], 7)
    feed_a(FEED_A[0])
    second = {}
    for j, da in enumerate(steps):
        p, q = first[da]
        keep(1, da, hi, mine(1, da, hi))
        keep(3, da, lo, mine(3, da, lo))
        p.wait_recv()
        keep(1, da, lo, mine(1, da, lo) + mid_p[j].astype(F32))
        sp = rcopy(at(1, da, all_k), end_p.at[j], b_next)
        q.wait_recv()
        keep(3, da, hi, mine(3, da, hi) + mid_m[j].astype(F32))
        sm = rcopy(at(3, da, all_k), end_m.at[j], b_prev)
        second[da] = (sp, sm)
        feed_a(FEED_A[1 + j])

    def summed(j, da):
        p, q = second[da]
        own = mine(0, da, all_k)
        p.wait_recv()
        own = own + end_p[j].astype(F32)
        q.wait_recv()
        return own + end_m[j].astype(F32)

    total[0] = summed(0, 2).astype(BF16)
    fp = rcopy(total.at[0, lo], imid.at[0], a_next)
    fm = rcopy(total.at[0, hi], imid.at[1], a_prev)
    feed_a(FEED_A[5])
    near_p = summed(1, 1)
    near_m = summed(2, 3)
    total[1, hi] = near_p[2:4].astype(BF16)
    total[2, lo] = near_m[0:2].astype(BF16)
    fp.wait_recv()
    total[1, lo] = (near_p[0:2] + imid[0].astype(F32)).astype(BF16)
    gp = rcopy(total.at[1], iend.at[0], a_next)
    fm.wait_recv()
    total[2, hi] = (near_m[2:4] + imid[1].astype(F32)).astype(BF16)
    gm = rcopy(total.at[2], iend.at[1], a_prev)
    feed_a(FEED_A[6])
    own = summed(3, 0)
    gp.wait_recv()
    own = own + iend[0].astype(F32)
    gm.wait_recv()
    own = own + iend[1].astype(F32)
    inner[...] = own.astype(BF16)
    base = m[0]
    for d in range(1, 4):
        for i in range(2):
            yy = (y + d) % 4
            rcopy(
                inner.at[(yy // 2) * 2 + i],
                last.at[d, c],
                device(x, yy // 2, yy % 2, z, i),
                base + 2 * (d - 1) + c,
            )
    near = rcopy(inner.at[yh * 2 + o], last.at[0, c], sib)
    feed_a(len(ORDER) - fed[1])

    def await_exchange(send, recv, buf):
        cp = pltpu.make_async_remote_copy(
            src_ref=buf.at[pl.ds(0, SLOTS - 1)],
            dst_ref=buf.at[pl.ds(0, SLOTS - 1)],
            send_sem=send,
            recv_sem=recv,
            device_id=sib,
            device_id_type=MESH,
        )
        cp.wait_send()
        cp.wait_recv()

    for cp in loads[3:]:
        cp.wait()
    mine_b.wait()
    await_exchange(bsend, brecv, arrived)
    inverse_b = (1.0 / counts_b[...].astype(F32)).T
    for t in range(TABLES):
        mean = arrived[slots[t]].astype(F32) * inverse_b[:, t : t + 1]
        st[:, E * (t + 1) : E * (t + 2)] = mean.astype(BF16)
    low_b = jnp.zeros((SAMP, RANK), F32)
    for j in range(WIDTH // BLK):
        cols = slice(BLK * j, BLK * (j + 1))
        low_b = low_b + jnp.dot(st[:, cols], v[cols, :], preferred_element_type=F32)
    low_b = low_b.astype(BF16)
    for j in range(WIDTH // BLK):
        cols = slice(BLK * j, BLK * (j + 1))
        wide = st[:, cols].astype(F32)
        projected = lax.dot_general(low_b, u[cols, :], OVER_COLS, preferred_element_type=F32)
        st[:, cols] = (wide * (projected + bias[0:1, cols]) + wide).astype(BF16)
    write = load(st, crossed_h, 8)

    near.wait_recv()
    for d in range(1, 4):
        for i in range(2):
            pltpu.make_async_remote_copy(
                src_ref=inner.at[0],
                dst_ref=last.at[d, i],
                send_sem=rsend.at[0],
                recv_sem=rrecv.at[base + 2 * (d - 1) + i],
                device_id=sib,
                device_id_type=MESH,
            ).wait_recv()
    ready = inner[k].astype(F32)
    for i in range(2):
        others = last[1, i].astype(F32) + last[2, i].astype(F32) + last[3, i].astype(F32)
        out[i] = others + jnp.where(c == i, ready, last[0, i].astype(F32))
    for cp in sent:
        cp.wait_send()
    home_a.wait()
    write.wait()
    await_exchange(asend, arecv, returned)


def step(slots, pooled, down, up, bias, stacked, upstream, counts_a, dense, counts_b):
    smem = pl.BlockSpec(memory_space=pltpu.SMEM)
    vmem = pl.BlockSpec(memory_space=pltpu.VMEM)
    anywhere = pl.BlockSpec(memory_space=pl.ANY)
    half = (2, PAD, RANK)
    whole = (4, PAD, RANK)
    return pl.pallas_call(
        step_kernel,
        out_shape=(
            jax.ShapeDtypeStruct((SAMP, WIDTH), BF16),
            jax.ShapeDtypeStruct((SAMP, E), BF16),
            jax.ShapeDtypeStruct((SLOTS, SAMP, E), BF16),
            jax.ShapeDtypeStruct((2, PAD, RANK), F32),
        ),
        in_specs=[smem] + [anywhere] * 9,
        out_specs=[anywhere, vmem, anywhere, vmem],
        scratch_shapes=[
            pltpu.SMEM((SLOTS,), jnp.int32),
            pltpu.VMEM((2, ROWS, RANK), BF16),
            pltpu.VMEM((1, ROWS), BF16),
            pltpu.VMEM((2, PAD, RANK), BF16),
            pltpu.VMEM((2, 4, 4, 4, PAD, RANK), BF16),
            pltpu.VMEM((WIDTH, RANK), BF16),
            pltpu.VMEM((WIDTH, RANK), BF16),
            pltpu.VMEM((1, WIDTH), F32),
            pltpu.VMEM((SAMP, WIDTH), BF16),
            pltpu.VMEM((SAMP, WIDTH), BF16),
            pltpu.VMEM((SAMP, WIDTH), BF16),
            pltpu.VMEM((WIDTH, RANK), BF16),
            pltpu.VMEM((WIDTH, RANK), BF16),
            pltpu.VMEM((1, WIDTH), F32),
            pltpu.VMEM((TABLES + 1, SAMP, E), BF16),
            pltpu.VMEM((SLOTS, SAMP, E), BF16),
            pltpu.VMEM((SLOTS, SAMP, E), BF16),
            pltpu.VMEM((SAMP, WIDTH), BF16),
            pltpu.VMEM((TABLES, SAMP), jnp.int32),
            pltpu.VMEM((TABLES, SAMP), jnp.int32),
            pltpu.VMEM((4, 4) + whole, BF16),
            pltpu.VMEM((4,) + half, BF16),
            pltpu.VMEM((4,) + half, BF16),
            pltpu.VMEM((4,) + whole, BF16),
            pltpu.VMEM((4,) + whole, BF16),
            pltpu.VMEM((3,) + whole, BF16),
            pltpu.VMEM((2,) + half, BF16),
            pltpu.VMEM((2,) + whole, BF16),
            pltpu.VMEM(whole, BF16),
            pltpu.VMEM((4, 2, PAD, RANK), BF16),
            pltpu.SemaphoreType.DMA((N_GATHER,)),
            pltpu.SemaphoreType.DMA((N_GATHER,)),
            pltpu.SemaphoreType.DMA((N_REDUCE,)),
            pltpu.SemaphoreType.DMA((N_REDUCE,)),
            pltpu.SemaphoreType.DMA((11,)),
            pltpu.SemaphoreType.DMA,
            pltpu.SemaphoreType.DMA,
            pltpu.SemaphoreType.DMA,
            pltpu.SemaphoreType.DMA,
        ],
        compiler_params=pltpu.CompilerParams(
            collective_id=1, has_side_effects=True, vmem_limit_bytes=62 << 20
        ),
        name="cross_step",
    )(slots, pooled, down, up, bias, stacked, upstream, counts_a, dense, counts_b)


PIECES = 8


def write_kernel(crossed, dense, returned, sums, crossed_o, dense_o, returned_o, down_o, up_o,
                 bias_o, crossed_v, dense_v, returned_v, sums_v, down_v, up_v, rsem, wsem):
    part = SLOTS // PIECES
    n = [0]

    def pair(src, mid, dst):
        i = n[0]
        n[0] += 1
        read = pltpu.make_async_copy(src, mid, rsem.at[i])
        read.start()
        return read, pltpu.make_async_copy(mid, dst, wsem.at[i])

    small = pltpu.make_async_copy(sums, sums_v, rsem.at[PIECES + 2])
    small.start()
    pairs = [pair(crossed, crossed_v, crossed_o), pair(dense, dense_v, dense_o)]
    for i in range(PIECES):
        at = pl.ds(part * i, part)
        pairs.append(pair(returned.at[at], returned_v.at[at], returned_o.at[at]))
    small.wait()
    down_v[...] = sums_v[0, 0:ROWS]
    up_v[...] = sums_v[1, 0:ROWS]
    bias_o[...] = sums_v[0, ROWS, 0:ROWS]
    writes = [
        pltpu.make_async_copy(down_v, down_o, wsem.at[PIECES + 2]),
        pltpu.make_async_copy(up_v, up_o, wsem.at[PIECES + 3]),
    ]
    for cp in writes:
        cp.start()
    for read, write in pairs:
        read.wait()
        write.start()
        writes.append(write)
    for cp in writes:
        cp.wait()


def write_out(crossed, dense, returned, sums):
    vmem = pl.BlockSpec(memory_space=pltpu.VMEM)
    anywhere = pl.BlockSpec(memory_space=pl.ANY)
    return pl.pallas_call(
        write_kernel,
        out_shape=(
            jax.ShapeDtypeStruct((SAMP, WIDTH), BF16),
            jax.ShapeDtypeStruct((SAMP, E), BF16),
            jax.ShapeDtypeStruct((SLOTS, SAMP, E), BF16),
            jax.ShapeDtypeStruct((ROWS, RANK), F32),
            jax.ShapeDtypeStruct((ROWS, RANK), F32),
            jax.ShapeDtypeStruct((ROWS,), F32),
        ),
        in_specs=[anywhere] * 4,
        out_specs=[anywhere] * 5 + [vmem],
        scratch_shapes=[
            pltpu.VMEM((SAMP, WIDTH), BF16),
            pltpu.VMEM((SAMP, E), BF16),
            pltpu.VMEM((SLOTS, SAMP, E), BF16),
            pltpu.VMEM((2, PAD, RANK), F32),
            pltpu.VMEM((ROWS, RANK), F32),
            pltpu.VMEM((ROWS, RANK), F32),
            pltpu.SemaphoreType.DMA((PIECES + 4,)),
            pltpu.SemaphoreType.DMA((PIECES + 4,)),
        ],
        compiler_params=pltpu.CompilerParams(vmem_limit_bytes=62 << 20),
        name="write_out",
    )(crossed, dense, returned, sums)


def local(
    pooled_b,
    dense_output_second,
    counts_b,
    slot_of,
    stacked_a,
    upstream_a,
    counts_a,
    down_projection,
    proj_up,
    cross_layer_bias,
):
    slots = slot_of[:TABLES]
    crossed_b, dense_gradient, returned, grad_down, grad_up, grad_bias = write_out(
        *step(
            slots,
            pooled_b[0],
            down_projection,
            jnp.transpose(proj_up),
            cross_layer_bias[None, :],
            stacked_a,
            upstream_a,
            jnp.transpose(counts_a),
            dense_output_second,
            jnp.transpose(counts_b),
        )
    )
    return (
        crossed_b,
        dense_gradient,
        returned[None],
        grad_down,
        jnp.transpose(grad_up),
        grad_bias,
    )


def solution(mesh):
    return jax.shard_map(
        local,
        mesh=mesh,
        in_specs=(
            P("wide", None, "pair", None),
            P(("wide", "pair"), None),
            P(("wide", "pair"), None),
            P(),
            P(("wide", "pair"), None),
            P(("wide", "pair"), None),
            P(("wide", "pair"), None),
            P("wide", None),
            P(None, "wide"),
            P("wide"),
        ),
        out_specs=(
            P(("wide", "pair"), None),
            P(("wide", "pair"), None),
            P("wide", None, "pair", None),
            P("wide", None),
            P(None, "wide"),
            P("wide"),
        ),
        check_vma=False,
    )
```

```python
import itertools

import jax
import jax.numpy as jnp
from jax import lax
from jax.experimental import pallas as pl
from jax.experimental.pallas import tpu as pltpu
from jax.sharding import PartitionSpec as P

MESH = pl.DeviceIdType.MESH
F32 = jnp.float32
BF16 = jnp.bfloat16

ROWS = 54
PAD = 56
RANK = 512
E = 128
TABLES = 26
SLOTS = 64
SAMP = 256
WIDTH = 3456
BLK = 384
OVER_ROWS = (((0,), (0,)), ((), ()))
OVER_COLS = (((1,), (1,)), ((), ()))


def place():
    w = lax.axis_index("wide")
    yl = lax.axis_index("pair")
    return w // 16, (w // 8) % 2, yl, (w // 2) % 4, w % 2


def device(x, yh, yl, z, c):
    return (((x * 2 + yh) * 4 + z) * 2 + c, yl)


def along_a(x, yh, yl, z, c, d):
    return device((x + d * (1 - c)) % 4, yh, yl, (z + d * c) % 4, c)


def along_b(x, yh, yl, z, c, d):
    return device((x + d * c) % 4, yh, yl, (z + d * (1 - c)) % 4, c)


def load_of(offset):
    dx, dy, dz, _ = offset
    loads = [0] * 6
    for d, at in ((dx, 0), (dz, 2)):
        if d % 2:
            loads[at + (d == 3)] += 1
        elif d:
            loads[at] += 1
            loads[at + 1] += 1
    if dy:
        loads[4] += 1
        loads[5] += 1
    return loads


def exchange_order():
    left = [o for o in itertools.product(range(4), range(2), range(4), range(2)) if any(o)]
    total, order = [0] * 6, []
    while left:

        def cost(offset):
            after = [p + q for p, q in zip(total, load_of(offset))]
            return max(after) - min(after), -sum(load_of(offset))

        best = min(left, key=cost)
        left.remove(best)
        order.append(best)
        total = [p + q for p, q in zip(total, load_of(best))]
    return order


ORDER = exchange_order()
N_GATHER = 3 + 4 + 16 + 16
N_REDUCE = 16 + 8 + 8 + 4 + 7
FEED_B = (0, 8, 5, 5, 5, 5, 5, 5, 5)
FEED_A = (4, 6, 6, 6, 6, 8, 8)


def target(me, offset):
    x, yh, _, z, c = me
    dx, dy, dz, dc = offset
    sx = dx + ((4 - dx) % 4 - dx) * c
    sz = dz + ((4 - dz) % 4 - dz) * c
    return ((((x + sx) % 4) * 2 + (yh + dy) % 2) * 4 + (z + sz) % 4) * 2 + (c + dc) % 2


def shard_of(m, w):
    x, yh, z, c = w // 16, (w // 8) % 2, (w // 2) % 4, w % 2
    return (m, z, x, yh * 2 + c) if m == 0 else (m, x, z, yh * 2 + c)


def step_kernel(slots, pooled, down_h, up_h, bias_h, stacked_h, upstream_h, counts_a_h, dense_h, counts_b_h,
                crossed_h, dense_g, returned, out,
                index, raw, raw_bias, shard, full, v, u, bias, stacked, upstream, pg, gv, gu, gb, tg, snd, arrived, st, counts_a,
                counts_b, sibling, mid_p, mid_m, end_p, end_m, total, imid, iend, inner, last,
                gsend, grecv, rsend, rrecv, local_sem, bsend, brecv, asend, arecv, x_sem, z_sem):
    place_of = place()
    x, yh, yl, z, c = place_of
    me = lax.axis_index("wide")
    o = 1 - c
    b = z * o + x * c
    a = x * o + z * c
    k = yh * 2 + c
    y = yh * 2 + yl
    sib = device(x, yh, yl, z, o)
    part = [device(x, 1 - yh, 1 - yl, z, i) for i in range(2)]
    a_next, a_prev = along_a(x, yh, yl, z, c, 1), along_a(x, yh, yl, z, c, 3)
    b_next, b_prev = along_b(x, yh, yl, z, c, 1), along_b(x, yh, yl, z, c, 3)
    lo, hi, all_k = pl.ds(0, 2), pl.ds(2, 2), pl.ds(0, 4)

    def load(src, dst, i):
        cp = pltpu.make_async_copy(src, dst, local_sem.at[i])
        cp.start()
        return cp

    loads = [
        load(stacked_h, stacked, 0),
        load(upstream_h, upstream, 1),
        load(counts_a_h, counts_a, 2),
        load(counts_b_h, counts_b, 3),
        load(dense_h, st.at[:, pl.ds(0, E)], 4),
    ]
    mine_b = load(pooled.at[me], arrived.at[me], 5)
    raws = [load(down_h, raw.at[0], 6), load(up_h, raw.at[1], 9), load(bias_h, raw_bias, 10)]

    barrier = pltpu.get_barrier_semaphore()
    x_line = [device((x + d) % 4, yh, yl, z, c) for d in range(1, 4)]
    z_line = [device(x, yh, yl, (z + d) % 4, c) for d in range(1, 4)]
    column = []
    for d in range(1, 4):
        yy = (y + d) % 4
        column += [device(x, yy // 2, yy % 2, z, i) for i in range(2)]

    def greet(sem, devices):
        for to in devices:
            pl.semaphore_signal(sem, inc=1, device_id=to, device_id_type=MESH)

    greet(barrier, [sib] + x_line + z_line + column)
    shard[...] = jnp.zeros_like(shard)
    for cp in raws:
        cp.wait()
    for i in range(2):
        shard[i, 0:ROWS] = raw[i]
    shard[0, ROWS : ROWS + 1, 0:ROWS] = raw_bias[...]
    pl.semaphore_wait(barrier, 13)
    greet(x_sem, x_line)

    fed = [0, 0]

    def feed_b(count):
        for offset in ORDER[fed[0] : fed[0] + count]:
            to = target(place_of, offset)
            pltpu.make_async_remote_copy(
                src_ref=pooled.at[to],
                dst_ref=arrived.at[me],
                send_sem=bsend,
                recv_sem=brecv,
                device_id=(to, yl),
                device_id_type=MESH,
            ).start()
        fed[0] += count

    def feed_a(count):
        for offset in ORDER[fed[1] : fed[1] + count]:
            to = target(place_of, offset)
            pltpu.make_async_remote_copy(
                src_ref=snd.at[to],
                dst_ref=returned.at[me],
                send_sem=asend,
                recv_sem=arecv,
                device_id=(to, yl),
                device_id_type=MESH,
            ).start()
        fed[1] += count

    n = [0]
    started = []

    def gcopy(src, dst, to, slot):
        cp = pltpu.make_async_remote_copy(
            src_ref=src,
            dst_ref=dst,
            send_sem=gsend.at[n[0]],
            recv_sem=grecv.at[slot],
            device_id=to,
            device_id_type=MESH,
        )
        n[0] += 1
        started.append(cp)
        cp.start()
        return cp

    s1 = []
    for i in range(2):
        bi, ai = (z, x) if i == 0 else (x, z)
        s1.append(gcopy(shard.at[i], full.at[i, bi, ai, k], part[i], 1 + (c + i) % 2))
    s1.append(gcopy(shard.at[o], full.at[o, a, b, k], sib, 0))

    @pl.loop(0, SLOTS)
    def _(s):
        held = jnp.int32(0)
        for t in range(TABLES):
            held = jnp.where(slots[t] == s, t + 1, held)
        index[s] = held

    full[c, b, a, k] = shard[c]
    pl.semaphore_wait(x_sem, 3)
    greet(z_sem, z_line)
    for cp in s1:
        cp.wait_recv()
    a_m, a_p, a_o = (a + 3) % 4, (a + 1) % 4, (a + 2) % 4
    b_m, b_p, b_o = (b + 3) % 4, (b + 1) % 4, (b + 2) % 4

    def ring(at, aa, to, slot, h=all_k):
        return gcopy(full.at[c, at, aa, h], full.at[c, at, aa, h], to, slot)

    outer = []

    def out_ring(j, aa):
        nxt = ring(b, aa, b_next, 7 + 4 * j)
        prv = ring(b, aa, b_prev, 8 + 4 * j)
        outer.append((aa, nxt, prv, 9 + 4 * j))

    across = []

    def over(bb, aa, j):
        across.append(ring(bb, aa, sib, 23 + j))

    up = ring(b, a, a_next, 3)
    down = ring(b, a, a_prev, 4)
    out_ring(0, a)
    pl.semaphore_wait(z_sem, 3)
    feed_b(FEED_B[0] + FEED_B[1])
    up.wait_recv()
    up2 = ring(b, a_m, a_next, 5, lo)
    out_ring(1, a_m)
    down.wait_recv()
    down2 = ring(b, a_p, a_prev, 6, hi)
    out_ring(2, a_p)
    over(b, a, 0)
    over(b, a_m, 1)
    over(b, a_p, 2)
    feed_b(FEED_B[2])
    up2.wait_recv()
    down2.wait_recv()
    out_ring(3, a_o)
    over(b, a_o, 3)
    feed_b(FEED_B[3])
    far = []
    for j, (aa, nxt, prv, slot) in enumerate(outer):
        nxt.wait_recv()
        n2 = ring(b_m, aa, b_next, slot, lo)
        over(b_m, aa, 4 + j)
        prv.wait_recv()
        p2 = ring(b_p, aa, b_prev, slot + 1, hi)
        over(b_p, aa, 8 + j)
        far.append((aa, n2, p2))
        feed_b(FEED_B[4 + j])
    for j, (aa, n2, p2) in enumerate(far):
        n2.wait_recv()
        p2.wait_recv()
        over(b_o, aa, 12 + j)
    feed_b(FEED_B[8])
    for cp in across:
        cp.wait_recv()
    for cp in started:
        cp.wait_send()
    feed_b(len(ORDER) - fed[0])

    for cp in loads[:3]:
        cp.wait()
    for w in range(64):
        rows = slice(ROWS * w, ROWS * (w + 1))
        v[rows, :] = full[shard_of(0, w)][0:ROWS]
        u[rows, :] = full[shard_of(1, w)][0:ROWS]
        bias[0:1, rows] = full[shard_of(0, w)][ROWS : ROWS + 1, 0:ROWS].astype(F32)
    low = jnp.zeros((SAMP, RANK), F32)
    lg = jnp.zeros((SAMP, RANK), F32)
    for j in range(WIDTH // BLK):
        cols = slice(BLK * j, BLK * (j + 1))
        sa = stacked[:, cols]
        scale = upstream[:, cols].astype(F32) * sa.astype(F32)
        gb[0:1, cols] = jnp.sum(scale, axis=0, keepdims=True)
        p = scale.astype(BF16)
        pg[:, cols] = p
        low = low + jnp.dot(sa, v[cols, :], preferred_element_type=F32)
        lg = lg + jnp.dot(p, u[cols, :], preferred_element_type=F32)
    low = low.astype(BF16)
    lg = lg.astype(BF16)
    tg[0] = jnp.zeros((SAMP, E), BF16)
    inverse = (1.0 / counts_a[...].astype(F32)).T
    for j in range(WIDTH // BLK):
        cols = slice(BLK * j, BLK * (j + 1))
        ua = upstream[:, cols].astype(F32)
        projected = lax.dot_general(low, u[cols, :], OVER_COLS, preferred_element_type=F32)
        through = lax.dot_general(lg, v[cols, :], OVER_COLS, preferred_element_type=F32)
        grad = ua * (projected + bias[0:1, cols]) + ua + through
        for i in range(BLK // E):
            t = j * (BLK // E) + i
            piece = grad[:, E * i : E * (i + 1)]
            if t == 0:
                dense_g[...] = piece.astype(BF16)
            else:
                tg[t] = (piece * inverse[:, t - 1 : t]).astype(BF16)
        gu[cols, :] = lax.dot_general(
            pg[:, cols], low, OVER_ROWS, preferred_element_type=F32
        ).astype(BF16)
        gv[cols, :] = lax.dot_general(
            stacked[:, cols], lg, OVER_ROWS, preferred_element_type=F32
        ).astype(BF16)
    for w in range(64):
        rows = slice(ROWS * w, ROWS * (w + 1))
        full[shard_of(0, w) + (slice(0, ROWS),)] = gv[rows, :]
        full[shard_of(1, w) + (slice(0, ROWS),)] = gu[rows, :]
        full[shard_of(0, w) + (slice(ROWS, ROWS + 1), slice(0, ROWS))] = gb[0:1, rows].astype(BF16)

    m = [0]
    sent = []

    def rcopy(src, dst, to, slot=None):
        cp = pltpu.make_async_remote_copy(
            src_ref=src,
            dst_ref=dst,
            send_sem=rsend.at[m[0]],
            recv_sem=rrecv.at[m[0] if slot is None else slot],
            device_id=to,
            device_id_type=MESH,
        )
        m[0] += 1
        sent.append(cp)
        cp.start()
        return cp

    steps = (2, 1, 3, 0)
    crossing = {}
    for db in steps:
        for da in steps:
            bb, aa = (a + db) % 4, (b + da) % 4
            crossing[db, da] = rcopy(full.at[o, bb, aa], sibling.at[bb, aa], sib)

    for s in range(SLOTS):
        snd[s] = tg[index[s]]
    got = set()

    def mine(db, da, h):
        if (db, da) not in got:
            crossing[db, da].wait_recv()
            got.add((db, da))
        bb, aa = (b + db) % 4, (a + da) % 4
        return full[c, bb, aa, h].astype(F32) + sibling[bb, aa, h].astype(F32)

    def keep(db, da, h, value):
        sibling[(b + db) % 4, (a + da) % 4, h] = value.astype(BF16)

    def at(db, da, h):
        return sibling.at[(b + db) % 4, (a + da) % 4, h]

    first = {}
    for j, da in enumerate(steps):
        keep(2, da, all_k, mine(2, da, all_k))
        first[da] = (
            rcopy(at(2, da, lo), mid_p.at[j], b_next),
            rcopy(at(2, da, hi), mid_m.at[j], b_prev),
        )
    home_a = load(snd.at[me], returned.at[me], 7)
    feed_a(FEED_A[0])
    second = {}
    for j, da in enumerate(steps):
        p, q = first[da]
        keep(1, da, hi, mine(1, da, hi))
        keep(3, da, lo, mine(3, da, lo))
        p.wait_recv()
        keep(1, da, lo, mine(1, da, lo) + mid_p[j].astype(F32))
        sp = rcopy(at(1, da, all_k), end_p.at[j], b_next)
        q.wait_recv()
        keep(3, da, hi, mine(3, da, hi) + mid_m[j].astype(F32))
        sm = rcopy(at(3, da, all_k), end_m.at[j], b_prev)
        second[da] = (sp, sm)
        feed_a(FEED_A[1 + j])

    def summed(j, da):
        p, q = second[da]
        own = mine(0, da, all_k)
        p.wait_recv()
        own = own + end_p[j].astype(F32)
        q.wait_recv()
        return own + end_m[j].astype(F32)

    total[0] = summed(0, 2).astype(BF16)
    fp = rcopy(total.at[0, lo], imid.at[0], a_next)
    fm = rcopy(total.at[0, hi], imid.at[1], a_prev)
    feed_a(FEED_A[5])
    near_p = summed(1, 1)
    near_m = summed(2, 3)
    total[1, hi] = near_p[2:4].astype(BF16)
    total[2, lo] = near_m[0:2].astype(BF16)
    fp.wait_recv()
    total[1, lo] = (near_p[0:2] + imid[0].astype(F32)).astype(BF16)
    gp = rcopy(total.at[1], iend.at[0], a_next)
    fm.wait_recv()
    total[2, hi] = (near_m[2:4] + imid[1].astype(F32)).astype(BF16)
    gm = rcopy(total.at[2], iend.at[1], a_prev)
    feed_a(FEED_A[6])
    own = summed(3, 0)
    gp.wait_recv()
    own = own + iend[0].astype(F32)
    gm.wait_recv()
    own = own + iend[1].astype(F32)
    inner[...] = own.astype(BF16)
    base = m[0]
    for d in range(1, 4):
        for i in range(2):
            yy = (y + d) % 4
            rcopy(
                inner.at[(yy // 2) * 2 + i],
                last.at[d, c],
                device(x, yy // 2, yy % 2, z, i),
                base + 2 * (d - 1) + c,
            )
    near = rcopy(inner.at[yh * 2 + o], last.at[0, c], sib)
    feed_a(len(ORDER) - fed[1])

    def await_exchange(send, recv, buf):
        cp = pltpu.make_async_remote_copy(
            src_ref=buf.at[pl.ds(0, SLOTS - 1)],
            dst_ref=buf.at[pl.ds(0, SLOTS - 1)],
            send_sem=send,
            recv_sem=recv,
            device_id=sib,
            device_id_type=MESH,
        )
        cp.wait_send()
        cp.wait_recv()

    for cp in loads[3:]:
        cp.wait()
    mine_b.wait()
    await_exchange(bsend, brecv, arrived)
    inverse_b = (1.0 / counts_b[...].astype(F32)).T
    for t in range(TABLES):
        mean = arrived[slots[t]].astype(F32) * inverse_b[:, t : t + 1]
        st[:, E * (t + 1) : E * (t + 2)] = mean.astype(BF16)
    low_b = jnp.zeros((SAMP, RANK), F32)
    for j in range(WIDTH // BLK):
        cols = slice(BLK * j, BLK * (j + 1))
        low_b = low_b + jnp.dot(st[:, cols], v[cols, :], preferred_element_type=F32)
    low_b = low_b.astype(BF16)
    for j in range(WIDTH // BLK):
        cols = slice(BLK * j, BLK * (j + 1))
        wide = st[:, cols].astype(F32)
        projected = lax.dot_general(low_b, u[cols, :], OVER_COLS, preferred_element_type=F32)
        st[:, cols] = (wide * (projected + bias[0:1, cols]) + wide).astype(BF16)
    write = load(st, crossed_h, 8)

    near.wait_recv()
    for d in range(1, 4):
        for i in range(2):
            pltpu.make_async_remote_copy(
                src_ref=inner.at[0],
                dst_ref=last.at[d, i],
                send_sem=rsend.at[0],
                recv_sem=rrecv.at[base + 2 * (d - 1) + i],
                device_id=sib,
                device_id_type=MESH,
            ).wait_recv()
    ready = inner[k].astype(F32)
    for i in range(2):
        others = last[1, i].astype(F32) + last[2, i].astype(F32) + last[3, i].astype(F32)
        out[i] = others + jnp.where(c == i, ready, last[0, i].astype(F32))
    for cp in sent:
        cp.wait_send()
    home_a.wait()
    write.wait()
    await_exchange(asend, arecv, returned)


def step(slots, pooled, down, up, bias, stacked, upstream, counts_a, dense, counts_b):
    smem = pl.BlockSpec(memory_space=pltpu.SMEM)
    vmem = pl.BlockSpec(memory_space=pltpu.VMEM)
    anywhere = pl.BlockSpec(memory_space=pl.ANY)
    half = (2, PAD, RANK)
    whole = (4, PAD, RANK)
    return pl.pallas_call(
        step_kernel,
        out_shape=(
            jax.ShapeDtypeStruct((SAMP, WIDTH), BF16),
            jax.ShapeDtypeStruct((SAMP, E), BF16),
            jax.ShapeDtypeStruct((SLOTS, SAMP, E), BF16),
            jax.ShapeDtypeStruct((2, PAD, RANK), F32),
        ),
        in_specs=[smem] + [anywhere] * 9,
        out_specs=[anywhere, vmem, anywhere, vmem],
        scratch_shapes=[
            pltpu.SMEM((SLOTS,), jnp.int32),
            pltpu.VMEM((2, ROWS, RANK), BF16),
            pltpu.VMEM((1, ROWS), BF16),
            pltpu.VMEM((2, PAD, RANK), BF16),
            pltpu.VMEM((2, 4, 4, 4, PAD, RANK), BF16),
            pltpu.VMEM((WIDTH, RANK), BF16),
            pltpu.VMEM((WIDTH, RANK), BF16),
            pltpu.VMEM((1, WIDTH), F32),
            pltpu.VMEM((SAMP, WIDTH), BF16),
            pltpu.VMEM((SAMP, WIDTH), BF16),
            pltpu.VMEM((SAMP, WIDTH), BF16),
            pltpu.VMEM((WIDTH, RANK), BF16),
            pltpu.VMEM((WIDTH, RANK), BF16),
            pltpu.VMEM((1, WIDTH), F32),
            pltpu.VMEM((TABLES + 1, SAMP, E), BF16),
            pltpu.VMEM((SLOTS, SAMP, E), BF16),
            pltpu.VMEM((SLOTS, SAMP, E), BF16),
            pltpu.VMEM((SAMP, WIDTH), BF16),
            pltpu.VMEM((TABLES, SAMP), jnp.int32),
            pltpu.VMEM((TABLES, SAMP), jnp.int32),
            pltpu.VMEM((4, 4) + whole, BF16),
            pltpu.VMEM((4,) + half, BF16),
            pltpu.VMEM((4,) + half, BF16),
            pltpu.VMEM((4,) + whole, BF16),
            pltpu.VMEM((4,) + whole, BF16),
            pltpu.VMEM((3,) + whole, BF16),
            pltpu.VMEM((2,) + half, BF16),
            pltpu.VMEM((2,) + whole, BF16),
            pltpu.VMEM(whole, BF16),
            pltpu.VMEM((4, 2, PAD, RANK), BF16),
            pltpu.SemaphoreType.DMA((N_GATHER,)),
            pltpu.SemaphoreType.DMA((N_GATHER,)),
            pltpu.SemaphoreType.DMA((N_REDUCE,)),
            pltpu.SemaphoreType.DMA((N_REDUCE,)),
            pltpu.SemaphoreType.DMA((11,)),
            pltpu.SemaphoreType.DMA,
            pltpu.SemaphoreType.DMA,
            pltpu.SemaphoreType.DMA,
            pltpu.SemaphoreType.DMA,
            pltpu.SemaphoreType.REGULAR,
            pltpu.SemaphoreType.REGULAR,
        ],
        compiler_params=pltpu.CompilerParams(
            collective_id=1, has_side_effects=True, vmem_limit_bytes=62 << 20
        ),
        name="cross_step",
    )(slots, pooled, down, up, bias, stacked, upstream, counts_a, dense, counts_b)


PIECES = 8


def write_kernel(crossed, dense, returned, sums, crossed_o, dense_o, returned_o, down_o, up_o,
                 bias_o, crossed_v, dense_v, returned_v, sums_v, down_v, up_v, rsem, wsem):
    part = SLOTS // PIECES
    n = [0]

    def pair(src, mid, dst):
        i = n[0]
        n[0] += 1
        read = pltpu.make_async_copy(src, mid, rsem.at[i])
        read.start()
        return read, pltpu.make_async_copy(mid, dst, wsem.at[i])

    small = pltpu.make_async_copy(sums, sums_v, rsem.at[PIECES + 2])
    small.start()
    pairs = [pair(crossed, crossed_v, crossed_o), pair(dense, dense_v, dense_o)]
    for i in range(PIECES):
        at = pl.ds(part * i, part)
        pairs.append(pair(returned.at[at], returned_v.at[at], returned_o.at[at]))
    small.wait()
    down_v[...] = sums_v[0, 0:ROWS]
    up_v[...] = sums_v[1, 0:ROWS]
    bias_o[...] = sums_v[0, ROWS, 0:ROWS]
    writes = [
        pltpu.make_async_copy(down_v, down_o, wsem.at[PIECES + 2]),
        pltpu.make_async_copy(up_v, up_o, wsem.at[PIECES + 3]),
    ]
    for cp in writes:
        cp.start()
    for read, write in pairs:
        read.wait()
        write.start()
        writes.append(write)
    for cp in writes:
        cp.wait()


def write_out(crossed, dense, returned, sums):
    vmem = pl.BlockSpec(memory_space=pltpu.VMEM)
    anywhere = pl.BlockSpec(memory_space=pl.ANY)
    return pl.pallas_call(
        write_kernel,
        out_shape=(
            jax.ShapeDtypeStruct((SAMP, WIDTH), BF16),
            jax.ShapeDtypeStruct((SAMP, E), BF16),
            jax.ShapeDtypeStruct((SLOTS, SAMP, E), BF16),
            jax.ShapeDtypeStruct((ROWS, RANK), F32),
            jax.ShapeDtypeStruct((ROWS, RANK), F32),
            jax.ShapeDtypeStruct((ROWS,), F32),
        ),
        in_specs=[anywhere] * 4,
        out_specs=[anywhere] * 5 + [vmem],
        scratch_shapes=[
            pltpu.VMEM((SAMP, WIDTH), BF16),
            pltpu.VMEM((SAMP, E), BF16),
            pltpu.VMEM((SLOTS, SAMP, E), BF16),
            pltpu.VMEM((2, PAD, RANK), F32),
            pltpu.VMEM((ROWS, RANK), F32),
            pltpu.VMEM((ROWS, RANK), F32),
            pltpu.SemaphoreType.DMA((PIECES + 4,)),
            pltpu.SemaphoreType.DMA((PIECES + 4,)),
        ],
        compiler_params=pltpu.CompilerParams(vmem_limit_bytes=62 << 20),
        name="write_out",
    )(crossed, dense, returned, sums)


def local(
    pooled_b,
    dense_output_second,
    counts_b,
    slot_of,
    stacked_a,
    upstream_a,
    counts_a,
    down_projection,
    proj_up,
    cross_layer_bias,
):
    slots = slot_of[:TABLES]
    crossed_b, dense_gradient, returned, grad_down, grad_up, grad_bias = write_out(
        *step(
            slots,
            pooled_b[0],
            down_projection,
            jnp.transpose(proj_up),
            cross_layer_bias[None, :],
            stacked_a,
            upstream_a,
            jnp.transpose(counts_a),
            dense_output_second,
            jnp.transpose(counts_b),
        )
    )
    return (
        crossed_b,
        dense_gradient,
        returned[None],
        grad_down,
        jnp.transpose(grad_up),
        grad_bias,
    )


def solution(mesh):
    return jax.shard_map(
        local,
        mesh=mesh,
        in_specs=(
            P("wide", None, "pair", None),
            P(("wide", "pair"), None),
            P(("wide", "pair"), None),
            P(),
            P(("wide", "pair"), None),
            P(("wide", "pair"), None),
            P(("wide", "pair"), None),
            P("wide", None),
            P(None, "wide"),
            P("wide"),
        ),
        out_specs=(
            P(("wide", "pair"), None),
            P(("wide", "pair"), None),
            P("wide", None, "pair", None),
            P("wide", None),
            P(None, "wide"),
            P("wide"),
        ),
        check_vma=False,
    )
```

```python
import itertools

import jax
import jax.numpy as jnp
from jax import lax
from jax.experimental import pallas as pl
from jax.experimental.pallas import tpu as pltpu
from jax.sharding import PartitionSpec as P

MESH = pl.DeviceIdType.MESH
F32 = jnp.float32
BF16 = jnp.bfloat16

ROWS = 54
PAD = 56
RANK = 512
E = 128
TABLES = 26
SLOTS = 64
SAMP = 256
WIDTH = 3456
BLK = 384
OVER_ROWS = (((0,), (0,)), ((), ()))
OVER_COLS = (((1,), (1,)), ((), ()))


def place():
    w = lax.axis_index("wide")
    yl = lax.axis_index("pair")
    return w // 16, (w // 8) % 2, yl, (w // 2) % 4, w % 2


def device(x, yh, yl, z, c):
    return (((x * 2 + yh) * 4 + z) * 2 + c, yl)


def along_a(x, yh, yl, z, c, d):
    return device((x + d * (1 - c)) % 4, yh, yl, (z + d * c) % 4, c)


def along_b(x, yh, yl, z, c, d):
    return device((x + d * c) % 4, yh, yl, (z + d * (1 - c)) % 4, c)


def load_of(offset):
    dx, dy, dz, _ = offset
    loads = [0] * 6
    for d, at in ((dx, 0), (dz, 2)):
        if d % 2:
            loads[at + (d == 3)] += 1
        elif d:
            loads[at] += 1
            loads[at + 1] += 1
    if dy:
        loads[4] += 1
        loads[5] += 1
    return loads


def exchange_order():
    left = [o for o in itertools.product(range(4), range(2), range(4), range(2)) if any(o)]
    total, order = [0] * 6, []
    while left:

        def cost(offset):
            after = [p + q for p, q in zip(total, load_of(offset))]
            return max(after) - min(after), -sum(load_of(offset))

        best = min(left, key=cost)
        left.remove(best)
        order.append(best)
        total = [p + q for p, q in zip(total, load_of(best))]
    return order


ORDER = exchange_order()
N_GATHER = 3 + 4 + 16 + 16
N_REDUCE = 16 + 8 + 8 + 4 + 7
FEED_B = (0, 8, 5, 5, 5, 5, 5, 5, 5)
FEED_A = (4, 6, 6, 6, 6, 8, 8)


def target(me, offset):
    x, yh, _, z, c = me
    dx, dy, dz, dc = offset
    sx = dx + ((4 - dx) % 4 - dx) * c
    sz = dz + ((4 - dz) % 4 - dz) * c
    return ((((x + sx) % 4) * 2 + (yh + dy) % 2) * 4 + (z + sz) % 4) * 2 + (c + dc) % 2


def shard_of(m, w):
    x, yh, z, c = w // 16, (w // 8) % 2, (w // 2) % 4, w % 2
    return (m, z, x, yh * 2 + c) if m == 0 else (m, x, z, yh * 2 + c)


def step_kernel(slots, pooled, down_h, up_h, bias_h, stacked_h, upstream_h, counts_a_h, dense_h, counts_b_h,
                crossed_h, dense_g, returned, out,
                index, raw, raw_bias, shard, full, v, u, bias, stacked, upstream, pg, gv, gu, gb, tg, snd, arrived, st, counts_a,
                counts_b, sibling, mid_p, mid_m, end_p, end_m, total, imid, iend, inner, last,
                gsend, grecv, rsend, rrecv, local_sem, bsend, brecv, asend, arecv, x_sem, z_sem):
    place_of = place()
    x, yh, yl, z, c = place_of
    me = lax.axis_index("wide")
    o = 1 - c
    b = z * o + x * c
    a = x * o + z * c
    k = yh * 2 + c
    y = yh * 2 + yl
    sib = device(x, yh, yl, z, o)
    part = [device(x, 1 - yh, 1 - yl, z, i) for i in range(2)]
    a_next, a_prev = along_a(x, yh, yl, z, c, 1), along_a(x, yh, yl, z, c, 3)
    b_next, b_prev = along_b(x, yh, yl, z, c, 1), along_b(x, yh, yl, z, c, 3)
    lo, hi, all_k = pl.ds(0, 2), pl.ds(2, 2), pl.ds(0, 4)

    def load(src, dst, i):
        cp = pltpu.make_async_copy(src, dst, local_sem.at[i])
        cp.start()
        return cp

    loads = [
        load(stacked_h, stacked, 0),
        load(upstream_h, upstream, 1),
        load(counts_a_h, counts_a, 2),
        load(counts_b_h, counts_b, 3),
        load(dense_h, st.at[:, pl.ds(0, E)], 4),
    ]
    mine_b = load(pooled.at[me], arrived.at[me], 5)
    raws = [load(down_h, raw.at[0], 6), load(up_h, raw.at[1], 9), load(bias_h, raw_bias, 10)]

    barrier = pltpu.get_barrier_semaphore()
    x_line = [device((x + d) % 4, yh, yl, z, c) for d in range(1, 4)]
    z_line = [device(x, yh, yl, (z + d) % 4, c) for d in range(1, 4)]
    column = []
    for d in range(1, 4):
        yy = (y + d) % 4
        column += [device(x, yy // 2, yy % 2, z, i) for i in range(2)]

    def greet(sem, devices):
        for to in devices:
            pl.semaphore_signal(sem, inc=1, device_id=to, device_id_type=MESH)

    greet(barrier, [sib] + x_line + z_line + column)
    shard[...] = jnp.zeros_like(shard)
    for cp in raws:
        cp.wait()
    for i in range(2):
        shard[i, 0:ROWS] = raw[i]
    shard[0, ROWS : ROWS + 1, 0:ROWS] = raw_bias[...]
    pl.semaphore_wait(barrier, 13)
    greet(x_sem, x_line)

    fed = [0, 0]

    def feed_b(count):
        for offset in ORDER[fed[0] : fed[0] + count]:
            to = target(place_of, offset)
            pltpu.make_async_remote_copy(
                src_ref=pooled.at[to],
                dst_ref=arrived.at[me],
                send_sem=bsend,
                recv_sem=brecv,
                device_id=(to, yl),
                device_id_type=MESH,
            ).start()
        fed[0] += count

    def feed_a(count):
        for offset in ORDER[fed[1] : fed[1] + count]:
            to = target(place_of, offset)
            pltpu.make_async_remote_copy(
                src_ref=snd.at[to],
                dst_ref=returned.at[me],
                send_sem=asend,
                recv_sem=arecv,
                device_id=(to, yl),
                device_id_type=MESH,
            ).start()
        fed[1] += count

    n = [0]
    started = []

    def gcopy(src, dst, to, slot):
        cp = pltpu.make_async_remote_copy(
            src_ref=src,
            dst_ref=dst,
            send_sem=gsend.at[n[0]],
            recv_sem=grecv.at[slot],
            device_id=to,
            device_id_type=MESH,
        )
        n[0] += 1
        started.append(cp)
        cp.start()
        return cp

    s1 = []
    for i in range(2):
        bi, ai = (z, x) if i == 0 else (x, z)
        s1.append(gcopy(shard.at[i], full.at[i, bi, ai, k], part[i], 1 + (c + i) % 2))
    s1.append(gcopy(shard.at[o], full.at[o, a, b, k], sib, 0))

    @pl.loop(0, SLOTS)
    def _(s):
        held = jnp.int32(0)
        for t in range(TABLES):
            held = jnp.where(slots[t] == s, t + 1, held)
        index[s] = held

    full[c, b, a, k] = shard[c]
    pl.semaphore_wait(x_sem, 3)
    greet(z_sem, z_line)
    for cp in s1:
        cp.wait_recv()
    a_m, a_p, a_o = (a + 3) % 4, (a + 1) % 4, (a + 2) % 4
    b_m, b_p, b_o = (b + 3) % 4, (b + 1) % 4, (b + 2) % 4

    def ring(at, aa, to, slot, h=all_k):
        return gcopy(full.at[c, at, aa, h], full.at[c, at, aa, h], to, slot)

    outer = []

    def out_ring(j, aa):
        nxt = ring(b, aa, b_next, 7 + 4 * j)
        prv = ring(b, aa, b_prev, 8 + 4 * j)
        outer.append((aa, nxt, prv, 9 + 4 * j))

    across = []

    def over(bb, aa, j):
        across.append(ring(bb, aa, sib, 23 + j))

    up = ring(b, a, a_next, 3)
    down = ring(b, a, a_prev, 4)
    far_a = ring(b, a, along_a(x, yh, yl, z, c, 2), 5)
    out_ring(0, a)
    pl.semaphore_wait(z_sem, 3)
    feed_b(FEED_B[0] + FEED_B[1])
    up.wait_recv()
    out_ring(1, a_m)
    down.wait_recv()
    out_ring(2, a_p)
    over(b, a, 0)
    over(b, a_m, 1)
    over(b, a_p, 2)
    feed_b(FEED_B[2])
    far_a.wait_recv()
    out_ring(3, a_o)
    over(b, a_o, 3)
    feed_b(FEED_B[3])
    far = []
    for j, (aa, nxt, prv, slot) in enumerate(outer):
        nxt.wait_recv()
        n2 = ring(b_m, aa, b_next, slot, lo)
        over(b_m, aa, 4 + j)
        prv.wait_recv()
        p2 = ring(b_p, aa, b_prev, slot + 1, hi)
        over(b_p, aa, 8 + j)
        far.append((aa, n2, p2))
        feed_b(FEED_B[4 + j])
    for j, (aa, n2, p2) in enumerate(far):
        n2.wait_recv()
        p2.wait_recv()
        over(b_o, aa, 12 + j)
    feed_b(FEED_B[8])
    for cp in across:
        cp.wait_recv()
    for cp in started:
        cp.wait_send()
    feed_b(len(ORDER) - fed[0])

    for cp in loads[:3]:
        cp.wait()
    for w in range(64):
        rows = slice(ROWS * w, ROWS * (w + 1))
        v[rows, :] = full[shard_of(0, w)][0:ROWS]
        u[rows, :] = full[shard_of(1, w)][0:ROWS]
        bias[0:1, rows] = full[shard_of(0, w)][ROWS : ROWS + 1, 0:ROWS].astype(F32)
    low = jnp.zeros((SAMP, RANK), F32)
    lg = jnp.zeros((SAMP, RANK), F32)
    for j in range(WIDTH // BLK):
        cols = slice(BLK * j, BLK * (j + 1))
        sa = stacked[:, cols]
        scale = upstream[:, cols].astype(F32) * sa.astype(F32)
        gb[0:1, cols] = jnp.sum(scale, axis=0, keepdims=True)
        p = scale.astype(BF16)
        pg[:, cols] = p
        low = low + jnp.dot(sa, v[cols, :], preferred_element_type=F32)
        lg = lg + jnp.dot(p, u[cols, :], preferred_element_type=F32)
    low = low.astype(BF16)
    lg = lg.astype(BF16)
    tg[0] = jnp.zeros((SAMP, E), BF16)
    inverse = (1.0 / counts_a[...].astype(F32)).T
    for j in range(WIDTH // BLK):
        cols = slice(BLK * j, BLK * (j + 1))
        ua = upstream[:, cols].astype(F32)
        projected = lax.dot_general(low, u[cols, :], OVER_COLS, preferred_element_type=F32)
        through = lax.dot_general(lg, v[cols, :], OVER_COLS, preferred_element_type=F32)
        grad = ua * (projected + bias[0:1, cols]) + ua + through
        for i in range(BLK // E):
            t = j * (BLK // E) + i
            piece = grad[:, E * i : E * (i + 1)]
            if t == 0:
                dense_g[...] = piece.astype(BF16)
            else:
                tg[t] = (piece * inverse[:, t - 1 : t]).astype(BF16)
        gu[cols, :] = lax.dot_general(
            pg[:, cols], low, OVER_ROWS, preferred_element_type=F32
        ).astype(BF16)
        gv[cols, :] = lax.dot_general(
            stacked[:, cols], lg, OVER_ROWS, preferred_element_type=F32
        ).astype(BF16)
    for w in range(64):
        rows = slice(ROWS * w, ROWS * (w + 1))
        full[shard_of(0, w) + (slice(0, ROWS),)] = gv[rows, :]
        full[shard_of(1, w) + (slice(0, ROWS),)] = gu[rows, :]
        full[shard_of(0, w) + (slice(ROWS, ROWS + 1), slice(0, ROWS))] = gb[0:1, rows].astype(BF16)

    m = [0]
    sent = []

    def rcopy(src, dst, to, slot=None):
        cp = pltpu.make_async_remote_copy(
            src_ref=src,
            dst_ref=dst,
            send_sem=rsend.at[m[0]],
            recv_sem=rrecv.at[m[0] if slot is None else slot],
            device_id=to,
            device_id_type=MESH,
        )
        m[0] += 1
        sent.append(cp)
        cp.start()
        return cp

    steps = (2, 1, 3, 0)
    crossing = {}
    for db in steps:
        for da in steps:
            bb, aa = (a + db) % 4, (b + da) % 4
            crossing[db, da] = rcopy(full.at[o, bb, aa], sibling.at[bb, aa], sib)

    for s in range(SLOTS):
        snd[s] = tg[index[s]]
    got = set()

    def mine(db, da, h):
        if (db, da) not in got:
            crossing[db, da].wait_recv()
            got.add((db, da))
        bb, aa = (b + db) % 4, (a + da) % 4
        return full[c, bb, aa, h].astype(F32) + sibling[bb, aa, h].astype(F32)

    def keep(db, da, h, value):
        sibling[(b + db) % 4, (a + da) % 4, h] = value.astype(BF16)

    def at(db, da, h):
        return sibling.at[(b + db) % 4, (a + da) % 4, h]

    first = {}
    for j, da in enumerate(steps):
        keep(2, da, all_k, mine(2, da, all_k))
        first[da] = (
            rcopy(at(2, da, lo), mid_p.at[j], b_next),
            rcopy(at(2, da, hi), mid_m.at[j], b_prev),
        )
    home_a = load(snd.at[me], returned.at[me], 7)
    feed_a(FEED_A[0])
    second = {}
    for j, da in enumerate(steps):
        p, q = first[da]
        keep(1, da, hi, mine(1, da, hi))
        keep(3, da, lo, mine(3, da, lo))
        p.wait_recv()
        keep(1, da, lo, mine(1, da, lo) + mid_p[j].astype(F32))
        sp = rcopy(at(1, da, all_k), end_p.at[j], b_next)
        q.wait_recv()
        keep(3, da, hi, mine(3, da, hi) + mid_m[j].astype(F32))
        sm = rcopy(at(3, da, all_k), end_m.at[j], b_prev)
        second[da] = (sp, sm)
        feed_a(FEED_A[1 + j])

    def summed(j, da):
        p, q = second[da]
        own = mine(0, da, all_k)
        p.wait_recv()
        own = own + end_p[j].astype(F32)
        q.wait_recv()
        return own + end_m[j].astype(F32)

    total[0] = summed(0, 2).astype(BF16)
    far_a = rcopy(total.at[0], imid, along_a(x, yh, yl, z, c, 2))
    feed_a(FEED_A[5])
    total[1] = summed(1, 1).astype(BF16)
    gp = rcopy(total.at[1], iend.at[0], a_next)
    total[2] = summed(2, 3).astype(BF16)
    gm = rcopy(total.at[2], iend.at[1], a_prev)
    feed_a(FEED_A[6])
    own = summed(3, 0)
    gp.wait_recv()
    own = own + iend[0].astype(F32)
    gm.wait_recv()
    own = own + iend[1].astype(F32)
    far_a.wait_recv()
    own = own + imid[...].astype(F32)
    inner[...] = own.astype(BF16)
    base = m[0]
    for d in range(1, 4):
        for i in range(2):
            yy = (y + d) % 4
            rcopy(
                inner.at[(yy // 2) * 2 + i],
                last.at[d, c],
                device(x, yy // 2, yy % 2, z, i),
                base + 2 * (d - 1) + c,
            )
    near = rcopy(inner.at[yh * 2 + o], last.at[0, c], sib)
    feed_a(len(ORDER) - fed[1])

    def await_exchange(send, recv, buf):
        cp = pltpu.make_async_remote_copy(
            src_ref=buf.at[pl.ds(0, SLOTS - 1)],
            dst_ref=buf.at[pl.ds(0, SLOTS - 1)],
            send_sem=send,
            recv_sem=recv,
            device_id=sib,
            device_id_type=MESH,
        )
        cp.wait_send()
        cp.wait_recv()

    for cp in loads[3:]:
        cp.wait()
    mine_b.wait()
    await_exchange(bsend, brecv, arrived)
    inverse_b = (1.0 / counts_b[...].astype(F32)).T
    for t in range(TABLES):
        mean = arrived[slots[t]].astype(F32) * inverse_b[:, t : t + 1]
        st[:, E * (t + 1) : E * (t + 2)] = mean.astype(BF16)
    low_b = jnp.zeros((SAMP, RANK), F32)
    for j in range(WIDTH // BLK):
        cols = slice(BLK * j, BLK * (j + 1))
        low_b = low_b + jnp.dot(st[:, cols], v[cols, :], preferred_element_type=F32)
    low_b = low_b.astype(BF16)
    for j in range(WIDTH // BLK):
        cols = slice(BLK * j, BLK * (j + 1))
        wide = st[:, cols].astype(F32)
        projected = lax.dot_general(low_b, u[cols, :], OVER_COLS, preferred_element_type=F32)
        st[:, cols] = (wide * (projected + bias[0:1, cols]) + wide).astype(BF16)
    write = load(st, crossed_h, 8)

    near.wait_recv()
    for d in range(1, 4):
        for i in range(2):
            pltpu.make_async_remote_copy(
                src_ref=inner.at[0],
                dst_ref=last.at[d, i],
                send_sem=rsend.at[0],
                recv_sem=rrecv.at[base + 2 * (d - 1) + i],
                device_id=sib,
                device_id_type=MESH,
            ).wait_recv()
    ready = inner[k].astype(F32)
    for i in range(2):
        others = last[1, i].astype(F32) + last[2, i].astype(F32) + last[3, i].astype(F32)
        out[i] = others + jnp.where(c == i, ready, last[0, i].astype(F32))
    for cp in sent:
        cp.wait_send()
    home_a.wait()
    write.wait()
    await_exchange(asend, arecv, returned)


def step(slots, pooled, down, up, bias, stacked, upstream, counts_a, dense, counts_b):
    smem = pl.BlockSpec(memory_space=pltpu.SMEM)
    vmem = pl.BlockSpec(memory_space=pltpu.VMEM)
    anywhere = pl.BlockSpec(memory_space=pl.ANY)
    half = (2, PAD, RANK)
    whole = (4, PAD, RANK)
    return pl.pallas_call(
        step_kernel,
        out_shape=(
            jax.ShapeDtypeStruct((SAMP, WIDTH), BF16),
            jax.ShapeDtypeStruct((SAMP, E), BF16),
            jax.ShapeDtypeStruct((SLOTS, SAMP, E), BF16),
            jax.ShapeDtypeStruct((2, PAD, RANK), F32),
        ),
        in_specs=[smem] + [anywhere] * 9,
        out_specs=[anywhere, vmem, anywhere, vmem],
        scratch_shapes=[
            pltpu.SMEM((SLOTS,), jnp.int32),
            pltpu.VMEM((2, ROWS, RANK), BF16),
            pltpu.VMEM((1, ROWS), BF16),
            pltpu.VMEM((2, PAD, RANK), BF16),
            pltpu.VMEM((2, 4, 4, 4, PAD, RANK), BF16),
            pltpu.VMEM((WIDTH, RANK), BF16),
            pltpu.VMEM((WIDTH, RANK), BF16),
            pltpu.VMEM((1, WIDTH), F32),
            pltpu.VMEM((SAMP, WIDTH), BF16),
            pltpu.VMEM((SAMP, WIDTH), BF16),
            pltpu.VMEM((SAMP, WIDTH), BF16),
            pltpu.VMEM((WIDTH, RANK), BF16),
            pltpu.VMEM((WIDTH, RANK), BF16),
            pltpu.VMEM((1, WIDTH), F32),
            pltpu.VMEM((TABLES + 1, SAMP, E), BF16),
            pltpu.VMEM((SLOTS, SAMP, E), BF16),
            pltpu.VMEM((SLOTS, SAMP, E), BF16),
            pltpu.VMEM((SAMP, WIDTH), BF16),
            pltpu.VMEM((TABLES, SAMP), jnp.int32),
            pltpu.VMEM((TABLES, SAMP), jnp.int32),
            pltpu.VMEM((4, 4) + whole, BF16),
            pltpu.VMEM((4,) + half, BF16),
            pltpu.VMEM((4,) + half, BF16),
            pltpu.VMEM((4,) + whole, BF16),
            pltpu.VMEM((4,) + whole, BF16),
            pltpu.VMEM((3,) + whole, BF16),
            pltpu.VMEM(whole, BF16),
            pltpu.VMEM((2,) + whole, BF16),
            pltpu.VMEM(whole, BF16),
            pltpu.VMEM((4, 2, PAD, RANK), BF16),
            pltpu.SemaphoreType.DMA((N_GATHER,)),
            pltpu.SemaphoreType.DMA((N_GATHER,)),
            pltpu.SemaphoreType.DMA((N_REDUCE,)),
            pltpu.SemaphoreType.DMA((N_REDUCE,)),
            pltpu.SemaphoreType.DMA((11,)),
            pltpu.SemaphoreType.DMA,
            pltpu.SemaphoreType.DMA,
            pltpu.SemaphoreType.DMA,
            pltpu.SemaphoreType.DMA,
            pltpu.SemaphoreType.REGULAR,
            pltpu.SemaphoreType.REGULAR,
        ],
        compiler_params=pltpu.CompilerParams(
            collective_id=1, has_side_effects=True, vmem_limit_bytes=62 << 20
        ),
        name="cross_step",
    )(slots, pooled, down, up, bias, stacked, upstream, counts_a, dense, counts_b)


PIECES = 8


def write_kernel(crossed, dense, returned, sums, crossed_o, dense_o, returned_o, down_o, up_o,
                 bias_o, crossed_v, dense_v, returned_v, sums_v, down_v, up_v, rsem, wsem):
    part = SLOTS // PIECES
    n = [0]

    def pair(src, mid, dst):
        i = n[0]
        n[0] += 1
        read = pltpu.make_async_copy(src, mid, rsem.at[i])
        read.start()
        return read, pltpu.make_async_copy(mid, dst, wsem.at[i])

    small = pltpu.make_async_copy(sums, sums_v, rsem.at[PIECES + 2])
    small.start()
    pairs = [pair(crossed, crossed_v, crossed_o), pair(dense, dense_v, dense_o)]
    for i in range(PIECES):
        at = pl.ds(part * i, part)
        pairs.append(pair(returned.at[at], returned_v.at[at], returned_o.at[at]))
    small.wait()
    down_v[...] = sums_v[0, 0:ROWS]
    up_v[...] = sums_v[1, 0:ROWS]
    bias_o[...] = sums_v[0, ROWS, 0:ROWS]
    writes = [
        pltpu.make_async_copy(down_v, down_o, wsem.at[PIECES + 2]),
        pltpu.make_async_copy(up_v, up_o, wsem.at[PIECES + 3]),
    ]
    for cp in writes:
        cp.start()
    for read, write in pairs:
        read.wait()
        write.start()
        writes.append(write)
    for cp in writes:
        cp.wait()


def write_out(crossed, dense, returned, sums):
    vmem = pl.BlockSpec(memory_space=pltpu.VMEM)
    anywhere = pl.BlockSpec(memory_space=pl.ANY)
    return pl.pallas_call(
        write_kernel,
        out_shape=(
            jax.ShapeDtypeStruct((SAMP, WIDTH), BF16),
            jax.ShapeDtypeStruct((SAMP, E), BF16),
            jax.ShapeDtypeStruct((SLOTS, SAMP, E), BF16),
            jax.ShapeDtypeStruct((ROWS, RANK), F32),
            jax.ShapeDtypeStruct((ROWS, RANK), F32),
            jax.ShapeDtypeStruct((ROWS,), F32),
        ),
        in_specs=[anywhere] * 4,
        out_specs=[anywhere] * 5 + [vmem],
        scratch_shapes=[
            pltpu.VMEM((SAMP, WIDTH), BF16),
            pltpu.VMEM((SAMP, E), BF16),
            pltpu.VMEM((SLOTS, SAMP, E), BF16),
            pltpu.VMEM((2, PAD, RANK), F32),
            pltpu.VMEM((ROWS, RANK), F32),
            pltpu.VMEM((ROWS, RANK), F32),
            pltpu.SemaphoreType.DMA((PIECES + 4,)),
            pltpu.SemaphoreType.DMA((PIECES + 4,)),
        ],
        compiler_params=pltpu.CompilerParams(vmem_limit_bytes=62 << 20),
        name="write_out",
    )(crossed, dense, returned, sums)


def local(
    pooled_b,
    dense_output_second,
    counts_b,
    slot_of,
    stacked_a,
    upstream_a,
    counts_a,
    down_projection,
    proj_up,
    cross_layer_bias,
):
    slots = slot_of[:TABLES]
    crossed_b, dense_gradient, returned, grad_down, grad_up, grad_bias = write_out(
        *step(
            slots,
            pooled_b[0],
            down_projection,
            jnp.transpose(proj_up),
            cross_layer_bias[None, :],
            stacked_a,
            upstream_a,
            jnp.transpose(counts_a),
            dense_output_second,
            jnp.transpose(counts_b),
        )
    )
    return (
        crossed_b,
        dense_gradient,
        returned[None],
        grad_down,
        jnp.transpose(grad_up),
        grad_bias,
    )


def solution(mesh):
    return jax.shard_map(
        local,
        mesh=mesh,
        in_specs=(
            P("wide", None, "pair", None),
            P(("wide", "pair"), None),
            P(("wide", "pair"), None),
            P(),
            P(("wide", "pair"), None),
            P(("wide", "pair"), None),
            P(("wide", "pair"), None),
            P("wide", None),
            P(None, "wide"),
            P("wide"),
        ),
        out_specs=(
            P(("wide", "pair"), None),
            P(("wide", "pair"), None),
            P("wide", None, "pair", None),
            P("wide", None),
            P(None, "wide"),
            P("wide"),
        ),
        check_vma=False,
    )
```
